16 devices in a mesh: sys: 2 (over y, z), blk: 8 (over x, core).
Axes of the slice: x: 4, y: 2, z: 1, core: 2. Of those that a mesh axis runs over, the one named last changes fastest.
The devices are a block of a 4x4x8 slice.
Arguments:
- positions: float32 [16384, 256], P(('sys', 'blk')), parts along dimension 0
- velocity: float32 [16384, 256], P(('sys', 'blk')), parts along dimension 0
- charges: float32 [16384], P(('sys', 'blk')), parts along dimension 0
Outputs:
- output 1: float32 [16384, 256], P(('sys', 'blk')), parts along dimension 0
- output 2: float32 [2], P('sys'), parts along dimension 0
- output 3: float32 [16384, 256], P(('sys', 'blk')), parts along dimension 0
- output 4: float32 [16384, 256], P(('sys', 'blk')), parts along dimension 0
There are 2 independent parts. The reference program is written for one: setup_inputs(seed, part) draws one part's arguments, and reference() takes and returns one part's arrays. A program takes and returns all parts, laid end to end along the dimension named above; each array names one.
All inputs are finite; a program needn't handle non-finite values.
Results may differ from the reference program's by a relative error of at most 0.00326424.
Values are sent between devices in bfloat16 or wider.
A program may use at most 768 MiB of HBM per device.

```python
import jax
import jax.numpy as jnp
from jax import lax

GROUP_SIZE = 8
ROWS = 1024
D = 256

N_PART = GROUP_SIZE * ROWS
ROW_TILE = 256
STEP_SIZE = 0.5
ELL_SQ = 1.0 * D
CHARGE_SCALE = (2.0 * D) ** 0.5 * N_PART ** -0.25


def setup_inputs(seed: int = 0, part: int = 0) -> dict:
    key = jax.random.fold_in(jax.random.key(seed), part)
    key_pos, key_spread, key_sign, key_mag, key_vel = jax.random.split(key, 5)
    spread = jax.random.uniform(key_spread, (N_PART, 1), jnp.float32, 0.5, 1.5)
    positions = jax.random.normal(key_pos, (N_PART, D), jnp.float32) * spread
    signs = (2 * jax.random.randint(key_sign, (N_PART,), 0, 2) - 1).astype(jnp.float32)
    charges = signs * jax.random.uniform(key_mag, (N_PART,), jnp.float32, 0.5, 1.5) * CHARGE_SCALE
    velocity = jax.random.normal(key_vel, (N_PART, D), jnp.float32)
    return {"positions": positions, "velocity": velocity, "charges": charges}


def kernel_forces(positions, charges):
    low = positions.astype(jnp.bfloat16)
    sq_norm = jnp.sum(jnp.square(low.astype(jnp.float32)), axis=1)
    col_ids = jnp.arange(N_PART)

    def tile_terms(tile_idx):
        row_start = tile_idx * ROW_TILE
        x_tile = lax.dynamic_slice_in_dim(low, row_start, ROW_TILE, 0)
        q_tile = lax.dynamic_slice_in_dim(charges, row_start, ROW_TILE, 0)
        sq_tile = lax.dynamic_slice_in_dim(sq_norm, row_start, ROW_TILE, 0)
        gram_tile = jnp.dot(x_tile, low.T, preferred_element_type=jnp.float32)
        dist_sq = jnp.maximum(sq_tile[:, None] + sq_norm[None, :] - 2.0 * gram_tile, 0.0)
        weight = q_tile[:, None] * charges[None, :] * jnp.exp(-dist_sq / (2.0 * ELL_SQ))
        on_diag = (row_start + jnp.arange(ROW_TILE))[:, None] == col_ids[None, :]
        weight = jnp.where(on_diag, 0.0, weight)
        pull_sum = jnp.dot(weight.astype(jnp.bfloat16), low, preferred_element_type=jnp.float32)
        force_tile = (jnp.sum(weight, axis=1)[:, None] * x_tile.astype(jnp.float32) - pull_sum) / ELL_SQ
        return force_tile, 0.5 * jnp.sum(weight)

    force_tiles, energy_tiles = lax.map(tile_terms, jnp.arange(N_PART // ROW_TILE))
    return force_tiles.reshape(N_PART, D), jnp.sum(energy_tiles)


def reference(positions, velocity, charges):
    force_zero, _ = kernel_forces(positions, charges)
    pos_one = positions + STEP_SIZE * velocity
    vel_one = velocity + STEP_SIZE * force_zero
    force_one, energy_one = kernel_forces(pos_one, charges)
    pos_two = pos_one + STEP_SIZE * vel_one
    vel_two = vel_one + STEP_SIZE * force_one
    return (force_one, energy_one.reshape(1), pos_two, vel_two)
```

```python
import functools
import math

import jax
import jax.numpy as jnp
from jax import lax
from jax.experimental import pallas as pl
from jax.experimental.pallas import tpu as pltpu
from jax.sharding import PartitionSpec as P

MESH = pl.DeviceIdType.MESH
STEP = 0.5
LOG2E = math.log2(math.e)
TILE = 256
LANES = 128
SIB, LEFT, RIGHT, LEFT_SIB, RIGHT_SIB, OPP, OPP_SIB = range(7)


def kernel(n, xs, vs, q_ref, f1_ref, e_ref, x2_ref, v2_ref,
           xg, mg, aw, qw, acc, rho, esend, ebuf,
           own_send, own_meta_send, fwd_send, fwd_meta_send, recv_sem, meta_recv, e_send, e_recv):
    rows, feat = xs.shape
    tiles = rows // TILE
    per = TILE // LANES
    half = tiles // 2
    me = lax.axis_index("blk")
    core = lax.rem(me, 2)
    sib = me + 1 - 2 * core
    right = lax.rem(me + 2, n)
    left = lax.rem(me + n - 2, n)
    opp = lax.rem(me + n // 2, n)
    left_sib = left + 1 - 2 * core
    right_sib = right + 1 - 2 * core
    opp_sib = opp + 1 - 2 * core

    def tile_rows(k):
        return pl.ds(k * TILE, TILE) if isinstance(k, int) else pl.ds(pl.multiple_of(k * TILE, TILE), TILE)

    def block_copy(e, k, blk, dev, send, rel):
        ref = xg.at[e, blk, tile_rows(k), :]
        return pltpu.make_async_remote_copy(src_ref=ref, dst_ref=ref, send_sem=send, recv_sem=recv_sem.at[rel, e, k],
                                            device_id={"blk": dev}, device_id_type=MESH)

    def meta_copy(blk, dev, send, rel):
        ref = mg.at[blk]
        return pltpu.make_async_remote_copy(src_ref=ref, dst_ref=ref, send_sem=send, recv_sem=meta_recv.at[rel],
                                            device_id={"blk": dev}, device_id_type=MESH)

    def own_copies(e, k):
        return (block_copy(e, k, me, right, own_send.at[0, e, k], LEFT),
                block_copy(e, k, me, left, own_send.at[1, e, k], RIGHT),
                block_copy(e, k, me, sib, own_send.at[2, e, k], SIB))

    def own_meta():
        return (meta_copy(me, right, own_meta_send.at[0], LEFT),
                meta_copy(me, left, own_meta_send.at[1], RIGHT),
                meta_copy(me, sib, own_meta_send.at[2], SIB))

    def fwd_left(e, k):
        return block_copy(e, k, left, sib, fwd_send.at[0, e, k], LEFT_SIB)

    def fwd_right(e, k):
        return block_copy(e, k, right, sib, fwd_send.at[1, e, k], RIGHT_SIB)

    def fwd_opp(e, k):
        return block_copy(e, k, opp, sib, fwd_send.at[2, e, k], OPP_SIB)

    def pass_right(e, k):
        return block_copy(e, k, left, right, fwd_send.at[3, e, k], OPP)

    def pass_left(e, k):
        return block_copy(e, k, right, left, fwd_send.at[3, e, k], OPP)

    def fwd_meta():
        return (meta_copy(left, sib, fwd_meta_send.at[0], LEFT_SIB),
                meta_copy(right, sib, fwd_meta_send.at[1], RIGHT_SIB),
                meta_copy(left, right, fwd_meta_send.at[2], OPP))

    def fwd_opp_meta():
        return meta_copy(opp, sib, fwd_meta_send.at[3], OPP_SIB)

    def arrived(e, k, blk, rel):
        block_copy(e, k, blk, sib, own_send.at[0, e, k], rel).wait_recv()

    def meta_arrived(blk, rel):
        meta_copy(blk, sib, own_meta_send.at[0], rel).wait_recv()

    def energy_copy(i):
        return pltpu.make_async_remote_copy(src_ref=esend, dst_ref=ebuf.at[me], send_sem=e_send.at[i], recv_sem=e_recv.at[i],
                                            device_id={"blk": lax.rem(me + i, n)}, device_id_type=MESH)

    def pair_tiles(e, pieces, masked):
        scale = LOG2E / feat
        cols = []
        for blk, k in pieces:
            b_j = xg[e, blk, tile_rows(k), :]
            a_j = jnp.concatenate([mg[blk, e, pl.ds(k * per + p, 1), :] for p in range(per)], axis=1)
            q_j = jnp.concatenate([mg[blk, 2, pl.ds(k * per + p, 1), :] for p in range(per)], axis=1)
            cols.append((b_j, a_j, q_j))
        for t in range(tiles):
            sl = tile_rows(t)
            x_t = xg[e, me, sl, :]
            a_t = jnp.concatenate([aw[e, sl, :]] * per, axis=1)
            q_t = jnp.concatenate([qw[sl, :]] * per, axis=1)
            rho_t = rho[e, sl, :]
            pull = None
            for p, (b_j, a_j, q_j) in enumerate(cols):
                g = lax.dot_general(x_t, b_j, (((1,), (1,)), ((), ())), preferred_element_type=jnp.float32)
                w = jnp.exp2(jnp.minimum(g * scale - a_t - a_j, 0.0)) * (q_t * q_j)
                if masked and p == t:
                    diag = lax.broadcasted_iota(jnp.int32, (TILE, TILE), 0) == lax.broadcasted_iota(jnp.int32, (TILE, TILE), 1)
                    w = jnp.where(diag, 0.0, w)
                for h in range(per):
                    rho_t = rho_t + w[:, h * LANES:(h + 1) * LANES]
                part = jnp.dot(w.astype(jnp.bfloat16), b_j, preferred_element_type=jnp.float32)
                pull = part if pull is None else pull + part
            rho[e, sl, :] = rho_t
            acc[e, sl, :] += pull

    def force(e, sl):
        rho_sum = jnp.sum(rho[e, sl, :], axis=1, keepdims=True)
        return (rho_sum * xg[e, me, sl, :].astype(jnp.float32) - acc[e, sl, :]) / feat

    barrier = pltpu.get_barrier_semaphore()
    for i in range(1, n):
        pl.semaphore_signal(barrier, inc=1, device_id={"blk": lax.rem(me + i, n)}, device_id_type=MESH)
    acc[...] = jnp.zeros_like(acc)
    rho[...] = jnp.zeros_like(rho)
    mg[me, 2] = q_ref[...]
    for k in range(tiles * per):
        qw[k * LANES:(k + 1) * LANES, :] = jnp.broadcast_to(q_ref[k:k + 1, :], (LANES, LANES)).T
    for k in range(tiles):
        sl = tile_rows(k)
        x1 = xs[sl, :] + STEP * vs[sl, :]
        xg[1, me, sl, :] = x1.astype(jnp.bfloat16)
        xg[0, me, sl, :] = xs[sl, :].astype(jnp.bfloat16)
        for e in (1, 0):
            b = xg[e, me, sl, :].astype(jnp.float32)
            s = jnp.sum(b * b, axis=1, keepdims=True) * (LOG2E / (2.0 * feat))
            aw[e, sl, :] = jnp.broadcast_to(s, (TILE, LANES))
            for p in range(per):
                r = k * per + p
                mg[me, e, r:r + 1, :] = aw[e, r * LANES:(r + 1) * LANES, :].T[0:1, :]
        if k == 0:
            pl.semaphore_wait(barrier, n - 1)
        for copy in own_copies(1, k):
            copy.start()
    for copy in own_meta():
        copy.start()
    for k in range(tiles):
        for copy in own_copies(0, k):
            copy.start()

    @pl.loop(0, 2)
    def _(i):
        pair_tiles(1 - i, [(me, k) for k in range(tiles)], True)

    meta_arrived(sib, SIB)

    @pl.loop(0, 2)
    def _(i):
        e = 1 - i
        for k in range(tiles):
            arrived(e, k, sib, SIB)
        pair_tiles(e, [(sib, k) for k in range(tiles)], False)

    meta_arrived(left, LEFT)
    meta_arrived(right, RIGHT)
    for copy in fwd_meta():
        copy.start()
    meta_arrived(left_sib, LEFT_SIB)
    meta_arrived(right_sib, RIGHT_SIB)

    @pl.loop(0, 2 * tiles)
    def _(i):
        e = 1 - i // tiles
        k = lax.rem(i, tiles)
        arrived(e, k, left, LEFT)
        fwd_left(e, k).start()

        @pl.when(k < half)
        def _():
            pass_right(e, k).start()

        arrived(e, k, right, RIGHT)
        fwd_right(e, k).start()

        @pl.when(k >= half)
        def _():
            pass_left(e, k).start()

        arrived(e, k, left_sib, LEFT_SIB)
        arrived(e, k, right_sib, RIGHT_SIB)
        pair_tiles(e, [(left, k), (right, k), (left_sib, k), (right_sib, k)], False)

    meta_arrived(opp, OPP)
    fwd_opp_meta().start()
    meta_arrived(opp_sib, OPP_SIB)

    def opposite(e, k):
        for t in (k, k + half):
            arrived(e, t, opp, OPP)
            fwd_opp(e, t).start()
        for t in (k, k + half):
            arrived(e, t, opp_sib, OPP_SIB)
        pair_tiles(e, [(opp, k), (opp, k + half), (opp_sib, k), (opp_sib, k + half)], False)

    @pl.loop(0, half)
    def _(k):
        opposite(1, k)

    part = jnp.zeros((8, LANES), jnp.float32)
    for r in range(rows // 8):
        part = part + rho[1, r * 8:(r + 1) * 8, :]
    esend[...] = part
    ebuf[me] = part
    for t in range(tiles):
        sl = tile_rows(t)
        f1_ref[sl, :] = force(1, sl)
    for i in range(1, n):
        energy_copy(i).start()

    @pl.loop(0, half)
    def _(k):
        opposite(0, k)

    for i in range(1, n):
        energy_copy(i).wait_recv()
    total = ebuf[0]
    for b in range(1, n):
        total = total + ebuf[b]
    e_ref[0] = 0.5 * jnp.sum(total)

    for t in range(tiles):
        sl = tile_rows(t)
        v1 = vs[sl, :] + STEP * force(0, sl)
        x2_ref[sl, :] = (xs[sl, :] + STEP * vs[sl, :]) + STEP * v1
        v2_ref[sl, :] = v1 + STEP * f1_ref[sl, :]

    for i in range(1, n):
        energy_copy(i).wait_send()
    for copy in own_meta() + fwd_meta() + (fwd_opp_meta(),):
        copy.wait_send()

    @pl.loop(0, 2 * tiles)
    def _(i):
        e = 1 - i // tiles
        k = lax.rem(i, tiles)
        for copy in own_copies(e, k) + (fwd_left(e, k), fwd_right(e, k), fwd_opp(e, k), pass_right(e, k)):
            copy.wait_send()


def solution(mesh):
    n = mesh.shape["blk"]
    row_spec = P(("sys", "blk"), None)
    vec_spec = P(("sys", "blk"))

    def local_steps(positions, velocity, charges):
        rows, feat = positions.shape
        tiles = rows // TILE
        block = jax.ShapeDtypeStruct((rows, feat), jnp.float32)
        vmem = pl.BlockSpec(memory_space=pltpu.VMEM)
        dma = pltpu.SemaphoreType.DMA
        force_one, energy_one, pos_two, vel_two = pl.pallas_call(
            functools.partial(kernel, n),
            out_shape=(block, jax.ShapeDtypeStruct((1,), jnp.float32), block, block),
            in_specs=[vmem, vmem, vmem],
            out_specs=(vmem, pl.BlockSpec(memory_space=pltpu.SMEM), vmem, vmem),
            scratch_shapes=[
                pltpu.VMEM((2, n, rows, feat), jnp.bfloat16),
                pltpu.VMEM((n, 3, rows // LANES, LANES), jnp.float32),
                pltpu.VMEM((2, rows, LANES), jnp.float32),
                pltpu.VMEM((rows, LANES), jnp.float32),
                pltpu.VMEM((2, rows, feat), jnp.float32),
                pltpu.VMEM((2, rows, LANES), jnp.float32),
                pltpu.VMEM((8, LANES), jnp.float32),
                pltpu.VMEM((n, 8, LANES), jnp.float32),
                dma((3, 2, tiles)),
                dma((3,)),
                dma((4, 2, tiles)),
                dma((4,)),
                dma((7, 2, tiles)),
                dma((7,)),
                dma((n,)),
                dma((n,)),
            ],
            compiler_params=pltpu.CompilerParams(collective_id=0, has_side_effects=True, vmem_limit_bytes=40 * 2**20),
            cost_estimate=pl.CostEstimate(flops=8 * n * rows * rows * feat, bytes_accessed=20 * rows * feat, transcendentals=2 * n * rows * rows),
        )(positions, velocity, charges.reshape(rows // LANES, LANES))
        return force_one, energy_one, pos_two, vel_two

    return jax.shard_map(local_steps, mesh=mesh, in_specs=(row_spec, row_spec, vec_spec), out_specs=(row_spec, P("sys"), row_spec, row_spec), check_vma=False)
```

```python
import functools
import math

import jax
import jax.numpy as jnp
from jax import lax
from jax.experimental import pallas as pl
from jax.experimental.pallas import tpu as pltpu
from jax.sharding import PartitionSpec as P

MESH = pl.DeviceIdType.MESH
STEP = 0.5
LOG2E = math.log2(math.e)
TILE = 256
LANES = 128
SIB, LEFT, RIGHT, LEFT_SIB, RIGHT_SIB, OPP, OPP_SIB = range(7)


def kernel(n, x0_hbm, v0_hbm, q_hbm, f1_ref, x2_ref, v2_ref, e_ref,
           xs, vs, q_ref, xg, mg, aw, qw, acc, rho, esend, ebuf,
           load_sem, q_sem, own_send, own_meta_send, fwd_send, fwd_meta_send, recv_sem, meta_recv, e_send, e_recv):
    rows, feat = xs.shape
    tiles = rows // TILE
    per = TILE // LANES
    half = tiles // 2
    me = lax.axis_index("blk")
    core = lax.rem(me, 2)
    sib = me + 1 - 2 * core
    right = lax.rem(me + 2, n)
    left = lax.rem(me + n - 2, n)
    opp = lax.rem(me + n // 2, n)
    left_sib = left + 1 - 2 * core
    right_sib = right + 1 - 2 * core
    opp_sib = opp + 1 - 2 * core

    def tile_rows(k):
        return pl.ds(k * TILE, TILE) if isinstance(k, int) else pl.ds(pl.multiple_of(k * TILE, TILE), TILE)

    def block_copy(e, k, blk, dev, send, rel):
        ref = xg.at[e, blk, tile_rows(k), :]
        return pltpu.make_async_remote_copy(src_ref=ref, dst_ref=ref, send_sem=send, recv_sem=recv_sem.at[rel, e, k],
                                            device_id={"blk": dev}, device_id_type=MESH)

    def meta_copy(blk, dev, send, rel):
        ref = mg.at[blk]
        return pltpu.make_async_remote_copy(src_ref=ref, dst_ref=ref, send_sem=send, recv_sem=meta_recv.at[rel],
                                            device_id={"blk": dev}, device_id_type=MESH)

    def own_copies(e, k):
        return (block_copy(e, k, me, right, own_send.at[0, e, k], LEFT),
                block_copy(e, k, me, left, own_send.at[1, e, k], RIGHT),
                block_copy(e, k, me, sib, own_send.at[2, e, k], SIB))

    def own_meta():
        return (meta_copy(me, right, own_meta_send.at[0], LEFT),
                meta_copy(me, left, own_meta_send.at[1], RIGHT),
                meta_copy(me, sib, own_meta_send.at[2], SIB))

    def fwd_left(e, k):
        return block_copy(e, k, left, sib, fwd_send.at[0, e, k], LEFT_SIB)

    def fwd_right(e, k):
        return block_copy(e, k, right, sib, fwd_send.at[1, e, k], RIGHT_SIB)

    def fwd_opp(e, k):
        return block_copy(e, k, opp, sib, fwd_send.at[2, e, k], OPP_SIB)

    def pass_right(e, k):
        return block_copy(e, k, left, right, fwd_send.at[3, e, k], OPP)

    def pass_left(e, k):
        return block_copy(e, k, right, left, fwd_send.at[3, e, k], OPP)

    def fwd_meta():
        return (meta_copy(left, sib, fwd_meta_send.at[0], LEFT_SIB),
                meta_copy(right, sib, fwd_meta_send.at[1], RIGHT_SIB),
                meta_copy(left, right, fwd_meta_send.at[2], OPP))

    def fwd_opp_meta():
        return meta_copy(opp, sib, fwd_meta_send.at[3], OPP_SIB)

    def arrived(e, k, blk, rel):
        block_copy(e, k, blk, sib, own_send.at[0, e, k], rel).wait_recv()

    def meta_arrived(blk, rel):
        meta_copy(blk, sib, own_meta_send.at[0], rel).wait_recv()

    def energy_copy(i):
        return pltpu.make_async_remote_copy(src_ref=esend, dst_ref=ebuf.at[me], send_sem=e_send.at[i], recv_sem=e_recv.at[i],
                                            device_id={"blk": lax.rem(me + i, n)}, device_id_type=MESH)

    def load(k, which):
        src, dst = ((x0_hbm, xs), (v0_hbm, vs))[which]
        return pltpu.make_async_copy(src.at[tile_rows(k), :], dst.at[tile_rows(k), :], load_sem.at[which, k])

    def pair_tiles(e, pieces, masked=False, finish=None):
        scale = LOG2E / feat
        cols = []
        for blk, k in pieces:
            b_j = xg[e, blk, tile_rows(k), :]
            a_j = jnp.concatenate([mg[blk, e, pl.ds(k * per + p, 1), :] for p in range(per)], axis=1)
            q_j = jnp.concatenate([mg[blk, 2, pl.ds(k * per + p, 1), :] for p in range(per)], axis=1)
            cols.append((b_j, a_j, q_j))
        for t in range(tiles):
            sl = tile_rows(t)
            x_t = xg[e, me, sl, :]
            a_t = jnp.concatenate([aw[e, sl, :]] * per, axis=1)
            q_t = jnp.concatenate([qw[sl, :]] * per, axis=1)
            rho_t = rho[e, sl, :]
            pull = None
            for p, (b_j, a_j, q_j) in enumerate(cols):
                g = lax.dot_general(x_t, b_j, (((1,), (1,)), ((), ())), preferred_element_type=jnp.float32)
                w = jnp.exp2(jnp.minimum(g * scale - a_t - a_j, 0.0)) * (q_t * q_j)
                if masked and p == t:
                    diag = lax.broadcasted_iota(jnp.int32, (TILE, TILE), 0) == lax.broadcasted_iota(jnp.int32, (TILE, TILE), 1)
                    w = jnp.where(diag, 0.0, w)
                for h in range(per):
                    rho_t = rho_t + w[:, h * LANES:(h + 1) * LANES]
                part = jnp.dot(w.astype(jnp.bfloat16), b_j, preferred_element_type=jnp.float32)
                pull = part if pull is None else pull + part
            pull = acc[e, sl, :] + pull
            if finish is None:
                rho[e, sl, :] = rho_t
                acc[e, sl, :] = pull
            else:
                finish(sl, force(e, sl, rho_t, pull))

    def force(e, sl, rho_t, pull):
        rho_sum = jnp.sum(rho_t, axis=1, keepdims=True)
        return (rho_sum * xg[e, me, sl, :].astype(jnp.float32) - pull) / feat

    barrier = pltpu.get_barrier_semaphore()
    for i in range(1, n):
        pl.semaphore_signal(barrier, inc=1, device_id={"blk": lax.rem(me + i, n)}, device_id_type=MESH)
    for k in range(tiles):
        load(k, 0).start()
        load(k, 1).start()
    q_load = pltpu.make_async_copy(q_hbm, q_ref, q_sem)
    q_load.start()
    acc[...] = jnp.zeros_like(acc)
    rho[...] = jnp.zeros_like(rho)
    for k in range(tiles):
        sl = tile_rows(k)
        load(k, 0).wait()
        load(k, 1).wait()
        x1 = xs[sl, :] + STEP * vs[sl, :]
        xg[1, me, sl, :] = x1.astype(jnp.bfloat16)
        xg[0, me, sl, :] = xs[sl, :].astype(jnp.bfloat16)
        if k == 0:
            pl.semaphore_wait(barrier, n - 1)
        for copy in own_copies(1, k):
            copy.start()
    q_load.wait()
    mg[me, 2] = q_ref[...]
    for k in range(tiles * per):
        sl = slice(k * LANES, (k + 1) * LANES)
        qw[sl, :] = jnp.broadcast_to(q_ref[k:k + 1, :], (LANES, LANES)).T
        for e in (1, 0):
            b = xg[e, me, sl, :].astype(jnp.float32)
            s = jnp.sum(b * b, axis=1, keepdims=True) * (LOG2E / (2.0 * feat))
            wide = jnp.broadcast_to(s, (LANES, LANES))
            aw[e, sl, :] = wide
            mg[me, e, k:k + 1, :] = wide.T[0:1, :]
    for k in range(tiles):
        for copy in own_copies(0, k):
            copy.start()
        if k == 0:
            for copy in own_meta():
                copy.start()

    @pl.loop(0, 2)
    def _(i):
        pair_tiles(1 - i, [(me, k) for k in range(tiles)], masked=True)

    meta_arrived(sib, SIB)

    @pl.loop(0, 2)
    def _(i):
        e = 1 - i
        for k in range(tiles):
            arrived(e, k, sib, SIB)
        pair_tiles(e, [(sib, k) for k in range(tiles)])

    def receive_sides(i):
        e, k = 1 - i // tiles, lax.rem(i, tiles)
        arrived(e, k, left, LEFT)
        fwd_left(e, k).start()

        @pl.when(k < half)
        def _():
            pass_right(e, k).start()

        arrived(e, k, right, RIGHT)
        fwd_right(e, k).start()

        @pl.when(k >= half)
        def _():
            pass_left(e, k).start()

    def compute_sides(i):
        e, k = 1 - i // tiles, lax.rem(i, tiles)
        arrived(e, k, left_sib, LEFT_SIB)
        arrived(e, k, right_sib, RIGHT_SIB)
        pair_tiles(e, [(left, k), (right, k), (left_sib, k), (right_sib, k)])

    def receive_opposite(e, k):
        for t in (k, k + half):
            arrived(e, t, opp, OPP)
            fwd_opp(e, t).start()

    def opposite_relayed(e, k):
        for t in (k, k + half):
            arrived(e, t, opp_sib, OPP_SIB)

    def compute_opposite(e, k):
        opposite_relayed(e, k)
        pair_tiles(e, [(opp, k), (opp, k + half), (opp_sib, k), (opp_sib, k + half)])

    meta_arrived(left, LEFT)
    meta_arrived(right, RIGHT)
    for copy in fwd_meta():
        copy.start()
    receive_sides(0)
    meta_arrived(left_sib, LEFT_SIB)
    meta_arrived(right_sib, RIGHT_SIB)

    @pl.loop(1, 2 * tiles + 1)
    def _(i):
        @pl.when(i < 2 * tiles)
        def _():
            receive_sides(i)

        @pl.when(i == 2 * tiles)
        def _():
            meta_arrived(opp, OPP)
            fwd_opp_meta().start()
            receive_opposite(1, 0)
            meta_arrived(opp_sib, OPP_SIB)

        compute_sides(i - 1)

    @pl.loop(1, 2 * half)
    def _(i):
        receive_opposite(1 - i // half, lax.rem(i, half))
        compute_opposite(1 - (i - 1) // half, lax.rem(i - 1, half))

        @pl.when(i == half)
        def _():
            part = jnp.zeros((8, LANES), jnp.float32)
            for r in range(rows // 8):
                part = part + rho[1, r * 8:(r + 1) * 8, :]
            esend[...] = part
            ebuf[me] = part
            for t in range(tiles):
                sl = tile_rows(t)
                f1_ref[sl, :] = force(1, sl, rho[1, sl, :], acc[1, sl, :])
            for p in range(1, n):
                energy_copy(p).start()

    last = half - 1
    pair_tiles(0, [(opp, last), (opp, last + half)])
    for i in range(1, n):
        energy_copy(i).wait_recv()
    total = ebuf[0]
    for b in range(1, n):
        total = total + ebuf[b]
    e_ref[...] = total
    opposite_relayed(0, last)

    def finish(sl, f0):
        v1 = vs[sl, :] + STEP * f0
        x2_ref[sl, :] = (xs[sl, :] + STEP * vs[sl, :]) + STEP * v1
        v2_ref[sl, :] = v1 + STEP * f1_ref[sl, :]

    pair_tiles(0, [(opp_sib, last), (opp_sib, last + half)], finish=finish)

    for i in range(1, n):
        energy_copy(i).wait_send()
    for copy in own_meta() + fwd_meta() + (fwd_opp_meta(),):
        copy.wait_send()

    @pl.loop(0, 2 * tiles)
    def _(i):
        e = 1 - i // tiles
        k = lax.rem(i, tiles)
        for copy in own_copies(e, k) + (fwd_left(e, k), fwd_right(e, k), fwd_opp(e, k), pass_right(e, k)):
            copy.wait_send()


def write_out(f1_ref, x2_ref, v2_ref, parts_ref, f1_hbm, e_ref, x2_hbm, v2_hbm, sem):
    copies = [pltpu.make_async_copy(src, dst, sem.at[i])
              for i, (src, dst) in enumerate(((f1_ref, f1_hbm), (x2_ref, x2_hbm), (v2_ref, v2_hbm)))]
    for copy in copies:
        copy.start()
    e_ref[0] = 0.5 * jnp.sum(parts_ref[...])
    for copy in copies:
        copy.wait()


def solution(mesh):
    n = mesh.shape["blk"]
    row_spec = P(("sys", "blk"), None)
    vec_spec = P(("sys", "blk"))

    def local_steps(positions, velocity, charges):
        rows, feat = positions.shape
        tiles = rows // TILE
        block = jax.ShapeDtypeStruct((rows, feat), jnp.float32)
        vmem = pl.BlockSpec(memory_space=pltpu.VMEM)
        hbm = pl.BlockSpec(memory_space=pltpu.HBM)
        dma = pltpu.SemaphoreType.DMA
        parts = pl.pallas_call(
            functools.partial(kernel, n),
            out_shape=(block, block, block, jax.ShapeDtypeStruct((8, LANES), jnp.float32)),
            in_specs=[hbm, hbm, hbm],
            out_specs=(vmem, vmem, vmem, vmem),
            scratch_shapes=[
                pltpu.VMEM((rows, feat), jnp.float32),
                pltpu.VMEM((rows, feat), jnp.float32),
                pltpu.VMEM((rows // LANES, LANES), jnp.float32),
                pltpu.VMEM((2, n, rows, feat), jnp.bfloat16),
                pltpu.VMEM((n, 3, rows // LANES, LANES), jnp.float32),
                pltpu.VMEM((2, rows, LANES), jnp.float32),
                pltpu.VMEM((rows, LANES), jnp.float32),
                pltpu.VMEM((2, rows, feat), jnp.float32),
                pltpu.VMEM((2, rows, LANES), jnp.float32),
                pltpu.VMEM((8, LANES), jnp.float32),
                pltpu.VMEM((n, 8, LANES), jnp.float32),
                dma((2, tiles)),
                dma,
                dma((3, 2, tiles)),
                dma((3,)),
                dma((4, 2, tiles)),
                dma((4,)),
                dma((7, 2, tiles)),
                dma((7,)),
                dma((n,)),
                dma((n,)),
            ],
            compiler_params=pltpu.CompilerParams(collective_id=0, has_side_effects=True, vmem_limit_bytes=52800000),
            cost_estimate=pl.CostEstimate(flops=8 * n * rows * rows * feat, bytes_accessed=20 * rows * feat, transcendentals=2 * n * rows * rows),
        )(positions, velocity, charges.reshape(rows // LANES, LANES))
        force_one, energy_one, pos_two, vel_two = pl.pallas_call(
            write_out,
            out_shape=(block, jax.ShapeDtypeStruct((1,), jnp.float32), block, block),
            in_specs=[vmem] * 4,
            out_specs=(hbm, pl.BlockSpec(memory_space=pltpu.SMEM), hbm, hbm),
            scratch_shapes=[dma((3,))],
            compiler_params=pltpu.CompilerParams(vmem_limit_bytes=2**20),
        )(*parts)
        return force_one, energy_one, pos_two, vel_two

    return jax.shard_map(local_steps, mesh=mesh, in_specs=(row_spec, row_spec, vec_spec), out_specs=(row_spec, P("sys"), row_spec, row_spec), check_vma=False)
```

```python
import functools
import math

import jax
import jax.numpy as jnp
from jax import lax
from jax.experimental import pallas as pl
from jax.experimental.pallas import tpu as pltpu
from jax.sharding import PartitionSpec as P

MESH = pl.DeviceIdType.MESH
STEP = 0.5
LOG2E = math.log2(math.e)
TILE = 256
LANES = 128
SIB, LEFT, RIGHT, LEFT_SIB, RIGHT_SIB, OPP, OPP_SIB = range(7)


def kernel(n, x0_hbm, v0_hbm, q_hbm, f1_ref, x2_ref, v2_ref, e_ref,
           xs, vs, q_ref, xg, mg, aw, qw, acc, rho, esend, ebuf,
           load_sem, q_sem, own_send, own_meta_send, fwd_send, fwd_meta_send, recv_sem, meta_recv, e_send, e_recv):
    rows, feat = xs.shape
    tiles = rows // TILE
    per = TILE // LANES
    half = tiles // 2
    me = lax.axis_index("blk")
    core = lax.rem(me, 2)
    sib = me + 1 - 2 * core
    right = lax.rem(me + 2, n)
    left = lax.rem(me + n - 2, n)
    opp = lax.rem(me + n // 2, n)
    left_sib = left + 1 - 2 * core
    right_sib = right + 1 - 2 * core
    opp_sib = opp + 1 - 2 * core

    def tile_rows(k):
        return pl.ds(k * TILE, TILE) if isinstance(k, int) else pl.ds(pl.multiple_of(k * TILE, TILE), TILE)

    def block_copy(e, k, blk, dev, send, rel):
        ref = xg.at[e, blk, tile_rows(k), :]
        return pltpu.make_async_remote_copy(src_ref=ref, dst_ref=ref, send_sem=send, recv_sem=recv_sem.at[rel, e, k],
                                            device_id={"blk": dev}, device_id_type=MESH)

    def meta_copy(blk, dev, send, rel):
        ref = mg.at[blk]
        return pltpu.make_async_remote_copy(src_ref=ref, dst_ref=ref, send_sem=send, recv_sem=meta_recv.at[rel],
                                            device_id={"blk": dev}, device_id_type=MESH)

    def own_copies(e, k):
        return (block_copy(e, k, me, right, own_send.at[0, e, k], LEFT),
                block_copy(e, k, me, left, own_send.at[1, e, k], RIGHT),
                block_copy(e, k, me, sib, own_send.at[2, e, k], SIB))

    def own_meta():
        return (meta_copy(me, right, own_meta_send.at[0], LEFT),
                meta_copy(me, left, own_meta_send.at[1], RIGHT),
                meta_copy(me, sib, own_meta_send.at[2], SIB))

    def fwd_left(e, k):
        return block_copy(e, k, left, sib, fwd_send.at[0, e, k], LEFT_SIB)

    def fwd_right(e, k):
        return block_copy(e, k, right, sib, fwd_send.at[1, e, k], RIGHT_SIB)

    def fwd_opp(e, k):
        return block_copy(e, k, opp, sib, fwd_send.at[2, e, k], OPP_SIB)

    def pass_right(e, k):
        return block_copy(e, k, left, right, fwd_send.at[3, e, k], OPP)

    def pass_left(e, k):
        return block_copy(e, k, right, left, fwd_send.at[3, e, k], OPP)

    def fwd_meta():
        return (meta_copy(left, sib, fwd_meta_send.at[0], LEFT_SIB),
                meta_copy(right, sib, fwd_meta_send.at[1], RIGHT_SIB),
                meta_copy(left, right, fwd_meta_send.at[2], OPP))

    def fwd_opp_meta():
        return meta_copy(opp, sib, fwd_meta_send.at[3], OPP_SIB)

    def arrived(e, k, blk, rel):
        block_copy(e, k, blk, sib, own_send.at[0, e, k], rel).wait_recv()

    def meta_arrived(blk, rel):
        meta_copy(blk, sib, own_meta_send.at[0], rel).wait_recv()

    def energy_copy(i):
        return pltpu.make_async_remote_copy(src_ref=esend, dst_ref=ebuf.at[me], send_sem=e_send.at[i], recv_sem=e_recv.at[i],
                                            device_id={"blk": lax.rem(me + i, n)}, device_id_type=MESH)

    def load(k, which):
        src, dst = ((x0_hbm, xs), (v0_hbm, vs))[which]
        return pltpu.make_async_copy(src.at[tile_rows(k), :], dst.at[tile_rows(k), :], load_sem.at[which, k])

    def pair_tiles(e, pieces, masked=False, finish=None):
        scale = LOG2E / feat
        cols = []
        for blk, k in pieces:
            b_j = xg[e, blk, tile_rows(k), :]
            a_j = jnp.concatenate([mg[blk, e, pl.ds(k * per + p, 1), :] for p in range(per)], axis=1)
            q_j = jnp.concatenate([mg[blk, 2, pl.ds(k * per + p, 1), :] for p in range(per)], axis=1)
            cols.append((b_j, a_j, q_j))
        for t in range(tiles):
            sl = tile_rows(t)
            x_t = xg[e, me, sl, :]
            a_t = jnp.concatenate([aw[e, sl, :]] * per, axis=1)
            q_t = jnp.concatenate([qw[sl, :]] * per, axis=1)
            rho_t = rho[e, sl, :]
            pull = None
            for p, (b_j, a_j, q_j) in enumerate(cols):
                g = lax.dot_general(x_t, b_j, (((1,), (1,)), ((), ())), preferred_element_type=jnp.float32)
                w = jnp.exp2(jnp.minimum(g * scale - a_t - a_j, 0.0)) * (q_t * q_j)
                if masked and p == t:
                    diag = lax.broadcasted_iota(jnp.int32, (TILE, TILE), 0) == lax.broadcasted_iota(jnp.int32, (TILE, TILE), 1)
                    w = jnp.where(diag, 0.0, w)
                for h in range(per):
                    rho_t = rho_t + w[:, h * LANES:(h + 1) * LANES]
                part = jnp.dot(w.astype(jnp.bfloat16), b_j, preferred_element_type=jnp.float32)
                pull = part if pull is None else pull + part
            pull = acc[e, sl, :] + pull
            if finish is None:
                rho[e, sl, :] = rho_t
                acc[e, sl, :] = pull
            else:
                finish(sl, force(e, sl, rho_t, pull))

    def force(e, sl, rho_t, pull):
        rho_sum = jnp.sum(rho_t, axis=1, keepdims=True)
        return (rho_sum * xg[e, me, sl, :].astype(jnp.float32) - pull) / feat

    barrier = pltpu.get_barrier_semaphore()
    for i in range(1, n):
        pl.semaphore_signal(barrier, inc=1, device_id={"blk": lax.rem(me + i, n)}, device_id_type=MESH)
    for k in range(tiles):
        load(k, 0).start()
        load(k, 1).start()
    q_load = pltpu.make_async_copy(q_hbm, q_ref, q_sem)
    q_load.start()
    acc[...] = jnp.zeros_like(acc)
    rho[...] = jnp.zeros_like(rho)
    for k in range(tiles):
        sl = tile_rows(k)
        load(k, 0).wait()
        load(k, 1).wait()
        x1 = xs[sl, :] + STEP * vs[sl, :]
        xg[1, me, sl, :] = x1.astype(jnp.bfloat16)
        xg[0, me, sl, :] = xs[sl, :].astype(jnp.bfloat16)
        if k == 0:
            pl.semaphore_wait(barrier, n - 1)
            for copy in own_copies(1, k):
                copy.start()
    q_load.wait()
    mg[me, 2] = q_ref[...]
    for k in range(tiles * per):
        sl = slice(k * LANES, (k + 1) * LANES)
        for e in (1, 0):
            b = xg[e, me, sl, :].astype(jnp.float32)
            s = jnp.sum(b * b, axis=1, keepdims=True) * (LOG2E / (2.0 * feat))
            wide = jnp.broadcast_to(s, (LANES, LANES))
            aw[e, sl, :] = wide
            mg[me, e, k:k + 1, :] = wide.T[0:1, :]
    for k in range(1, tiles):
        for copy in own_copies(1, k):
            copy.start()
        if k == 1:
            for copy in own_meta():
                copy.start()
    for k in range(tiles):
        for copy in own_copies(0, k):
            copy.start()
    for k in range(tiles * per):
        qw[k * LANES:(k + 1) * LANES, :] = jnp.broadcast_to(q_ref[k:k + 1, :], (LANES, LANES)).T

    @pl.loop(0, 2)
    def _(i):
        pair_tiles(1 - i, [(me, k) for k in range(tiles)], masked=True)

    meta_arrived(sib, SIB)

    @pl.loop(0, 2)
    def _(i):
        e = 1 - i
        for k in range(tiles):
            arrived(e, k, sib, SIB)
        pair_tiles(e, [(sib, k) for k in range(tiles)])

    def receive_sides(i):
        e, k = 1 - i // tiles, lax.rem(i, tiles)
        arrived(e, k, left, LEFT)
        fwd_left(e, k).start()

        @pl.when(k < half)
        def _():
            pass_right(e, k).start()

        arrived(e, k, right, RIGHT)
        fwd_right(e, k).start()

        @pl.when(k >= half)
        def _():
            pass_left(e, k).start()

    def own_sides(i):
        e, k = 1 - i // tiles, lax.rem(i, tiles)
        pair_tiles(e, [(left, k), (right, k)])

    def relayed_sides(i):
        e, k = 1 - i // tiles, lax.rem(i, tiles)
        arrived(e, k, left_sib, LEFT_SIB)
        arrived(e, k, right_sib, RIGHT_SIB)
        pair_tiles(e, [(left_sib, k), (right_sib, k)])

    def receive_opposite(e, k):
        for t in (k, k + half):
            arrived(e, t, opp, OPP)
            fwd_opp(e, t).start()

    def own_opposite(e, k):
        pair_tiles(e, [(opp, k), (opp, k + half)])

    def relayed_opposite(e, k, finish=None):
        for t in (k, k + half):
            arrived(e, t, opp_sib, OPP_SIB)
        pair_tiles(e, [(opp_sib, k), (opp_sib, k + half)], finish=finish)

    meta_arrived(left, LEFT)
    meta_arrived(right, RIGHT)
    for copy in fwd_meta():
        copy.start()
    meta_arrived(left_sib, LEFT_SIB)
    meta_arrived(right_sib, RIGHT_SIB)

    @pl.loop(0, 2 * tiles)
    def _(i):
        receive_sides(i)

        @pl.when(i > 0)
        def _():
            relayed_sides(i - 1)

        own_sides(i)

    meta_arrived(opp, OPP)
    fwd_opp_meta().start()
    receive_opposite(1, 0)
    relayed_sides(2 * tiles - 1)
    meta_arrived(opp_sib, OPP_SIB)

    @pl.loop(0, 2 * half - 1)
    def _(i):
        e, k = 1 - i // half, lax.rem(i, half)

        @pl.when(i > 0)
        def _():
            receive_opposite(e, k)

        own_opposite(e, k)

        @pl.when(i == half)
        def _():
            part = jnp.zeros((8, LANES), jnp.float32)
            for r in range(rows // 8):
                part = part + rho[1, r * 8:(r + 1) * 8, :]
            esend[...] = part
            ebuf[me] = part
            for p in range(1, n):
                energy_copy(p).start()

        relayed_opposite(e, k)

    last = half - 1
    receive_opposite(0, last)
    own_opposite(0, last)
    for t in range(tiles):
        sl = tile_rows(t)
        f1_ref[sl, :] = force(1, sl, rho[1, sl, :], acc[1, sl, :])
    for i in range(1, n):
        energy_copy(i).wait_recv()
    total = ebuf[0]
    for b in range(1, n):
        total = total + ebuf[b]
    e_ref[...] = total

    def finish(sl, f0):
        v1 = vs[sl, :] + STEP * f0
        x2_ref[sl, :] = (xs[sl, :] + STEP * vs[sl, :]) + STEP * v1
        v2_ref[sl, :] = v1 + STEP * f1_ref[sl, :]

    relayed_opposite(0, last, finish=finish)

    for i in range(1, n):
        energy_copy(i).wait_send()
    for copy in own_meta() + fwd_meta() + (fwd_opp_meta(),):
        copy.wait_send()

    @pl.loop(0, 2 * tiles)
    def _(i):
        e = 1 - i // tiles
        k = lax.rem(i, tiles)
        for copy in own_copies(e, k) + (fwd_left(e, k), fwd_right(e, k), fwd_opp(e, k), pass_right(e, k)):
            copy.wait_send()


def write_out(f1_ref, x2_ref, v2_ref, parts_ref, f1_hbm, e_ref, x2_hbm, v2_hbm, sem):
    copies = [pltpu.make_async_copy(src, dst, sem.at[i])
              for i, (src, dst) in enumerate(((f1_ref, f1_hbm), (x2_ref, x2_hbm), (v2_ref, v2_hbm)))]
    for copy in copies:
        copy.start()
    e_ref[0] = 0.5 * jnp.sum(parts_ref[...])
    for copy in copies:
        copy.wait()


def solution(mesh):
    n = mesh.shape["blk"]
    row_spec = P(("sys", "blk"), None)
    vec_spec = P(("sys", "blk"))

    def local_steps(positions, velocity, charges):
        rows, feat = positions.shape
        tiles = rows // TILE
        block = jax.ShapeDtypeStruct((rows, feat), jnp.float32)
        vmem = pl.BlockSpec(memory_space=pltpu.VMEM)
        hbm = pl.BlockSpec(memory_space=pltpu.HBM)
        dma = pltpu.SemaphoreType.DMA
        parts = pl.pallas_call(
            functools.partial(kernel, n),
            out_shape=(block, block, block, jax.ShapeDtypeStruct((8, LANES), jnp.float32)),
            in_specs=[hbm, hbm, hbm],
            out_specs=(vmem, vmem, vmem, vmem),
            scratch_shapes=[
                pltpu.VMEM((rows, feat), jnp.float32),
                pltpu.VMEM((rows, feat), jnp.float32),
                pltpu.VMEM((rows // LANES, LANES), jnp.float32),
                pltpu.VMEM((2, n, rows, feat), jnp.bfloat16),
                pltpu.VMEM((n, 3, rows // LANES, LANES), jnp.float32),
                pltpu.VMEM((2, rows, LANES), jnp.float32),
                pltpu.VMEM((rows, LANES), jnp.float32),
                pltpu.VMEM((2, rows, feat), jnp.float32),
                pltpu.VMEM((2, rows, LANES), jnp.float32),
                pltpu.VMEM((8, LANES), jnp.float32),
                pltpu.VMEM((n, 8, LANES), jnp.float32),
                dma((2, tiles)),
                dma,
                dma((3, 2, tiles)),
                dma((3,)),
                dma((4, 2, tiles)),
                dma((4,)),
                dma((7, 2, tiles)),
                dma((7,)),
                dma((n,)),
                dma((n,)),
            ],
            compiler_params=pltpu.CompilerParams(collective_id=0, has_side_effects=True, vmem_limit_bytes=52800000),
            cost_estimate=pl.CostEstimate(flops=8 * n * rows * rows * feat, bytes_accessed=20 * rows * feat, transcendentals=2 * n * rows * rows),
        )(positions, velocity, charges.reshape(rows // LANES, LANES))
        force_one, energy_one, pos_two, vel_two = pl.pallas_call(
            write_out,
            out_shape=(block, jax.ShapeDtypeStruct((1,), jnp.float32), block, block),
            in_specs=[vmem] * 4,
            out_specs=(hbm, pl.BlockSpec(memory_space=pltpu.SMEM), hbm, hbm),
            scratch_shapes=[dma((3,))],
            compiler_params=pltpu.CompilerParams(vmem_limit_bytes=2**20),
        )(*parts)
        return force_one, energy_one, pos_two, vel_two

    return jax.shard_map(local_steps, mesh=mesh, in_specs=(row_spec, row_spec, vec_spec), out_specs=(row_spec, P("sys"), row_spec, row_spec), check_vma=False)
```

```python
import functools
import math

import jax
import jax.numpy as jnp
from jax import lax
from jax.experimental import pallas as pl
from jax.experimental.pallas import tpu as pltpu
from jax.sharding import PartitionSpec as P

MESH = pl.DeviceIdType.MESH
STEP = 0.5
LOG2E = math.log2(math.e)
TILE = 256
LANES = 128
SIB, LEFT, RIGHT, LEFT_SIB, RIGHT_SIB, OPP, OPP_SIB = range(7)


def kernel(n, x0_hbm, v0_hbm, q_hbm, f1_ref, x2_ref, v2_ref, e_ref,
           xs, vs, q_ref, xg, mg, aw, qw, acc, rho, esend, ebuf,
           load_sem, q_sem, own_send, own_meta_send, fwd_send, fwd_meta_send, recv_sem, meta_recv, e_send, e_recv):
    rows, feat = xs.shape
    tiles = rows // TILE
    per = TILE // LANES
    half = tiles // 2
    me = lax.axis_index("blk")
    core = lax.rem(me, 2)
    sib = me + 1 - 2 * core
    right = lax.rem(me + 2, n)
    left = lax.rem(me + n - 2, n)
    opp = lax.rem(me + n // 2, n)
    left_sib = left + 1 - 2 * core
    right_sib = right + 1 - 2 * core
    opp_sib = opp + 1 - 2 * core

    def tile_rows(k):
        return pl.ds(k * TILE, TILE) if isinstance(k, int) else pl.ds(pl.multiple_of(k * TILE, TILE), TILE)

    def block_copy(e, k, blk, dev, send, rel):
        ref = xg.at[e, blk, tile_rows(k), :]
        return pltpu.make_async_remote_copy(src_ref=ref, dst_ref=ref, send_sem=send, recv_sem=recv_sem.at[rel, e, k],
                                            device_id={"blk": dev}, device_id_type=MESH)

    def meta_copy(blk, dev, send, rel):
        ref = mg.at[blk]
        return pltpu.make_async_remote_copy(src_ref=ref, dst_ref=ref, send_sem=send, recv_sem=meta_recv.at[rel],
                                            device_id={"blk": dev}, device_id_type=MESH)

    def own_copies(e, k):
        return (block_copy(e, k, me, right, own_send.at[0, e, k], LEFT),
                block_copy(e, k, me, left, own_send.at[1, e, k], RIGHT),
                block_copy(e, k, me, sib, own_send.at[2, e, k], SIB))

    def own_meta():
        return (meta_copy(me, right, own_meta_send.at[0], LEFT),
                meta_copy(me, left, own_meta_send.at[1], RIGHT),
                meta_copy(me, sib, own_meta_send.at[2], SIB))

    def fwd_left(e, k):
        return block_copy(e, k, left, sib, fwd_send.at[0, e, k], LEFT_SIB)

    def fwd_right(e, k):
        return block_copy(e, k, right, sib, fwd_send.at[1, e, k], RIGHT_SIB)

    def fwd_opp(e, k):
        return block_copy(e, k, opp, sib, fwd_send.at[2, e, k], OPP_SIB)

    def pass_right(e, k):
        return block_copy(e, k, left, right, fwd_send.at[3, e, k], OPP)

    def pass_left(e, k):
        return block_copy(e, k, right, left, fwd_send.at[3, e, k], OPP)

    def fwd_meta():
        return (meta_copy(left, sib, fwd_meta_send.at[0], LEFT_SIB),
                meta_copy(right, sib, fwd_meta_send.at[1], RIGHT_SIB),
                meta_copy(left, right, fwd_meta_send.at[2], OPP))

    def fwd_opp_meta():
        return meta_copy(opp, sib, fwd_meta_send.at[3], OPP_SIB)

    def arrived(e, k, blk, rel):
        block_copy(e, k, blk, sib, own_send.at[0, e, k], rel).wait_recv()

    def meta_arrived(blk, rel):
        meta_copy(blk, sib, own_meta_send.at[0], rel).wait_recv()

    def energy_copy(i):
        return pltpu.make_async_remote_copy(src_ref=esend, dst_ref=ebuf.at[me], send_sem=e_send.at[i], recv_sem=e_recv.at[i],
                                            device_id={"blk": lax.rem(me + i, n)}, device_id_type=MESH)

    def load(k, which):
        src, dst = ((x0_hbm, xs), (v0_hbm, vs))[which]
        return pltpu.make_async_copy(src.at[tile_rows(k), :], dst.at[tile_rows(k), :], load_sem.at[which, k])

    def pair_tiles(e, pieces, masked=False, finish=None):
        scale = LOG2E / feat
        cols = []
        for blk, k in pieces:
            b_j = xg[e, blk, tile_rows(k), :]
            a_j = jnp.concatenate([mg[blk, e, pl.ds(k * per + p, 1), :] for p in range(per)], axis=1)
            q_j = jnp.concatenate([mg[blk, 2, pl.ds(k * per + p, 1), :] for p in range(per)], axis=1)
            cols.append((b_j, a_j, q_j))
        for t in range(tiles):
            sl = tile_rows(t)
            x_t = xg[e, me, sl, :]
            a_t = jnp.concatenate([aw[e, sl, :]] * per, axis=1)
            q_t = jnp.concatenate([qw[sl, :]] * per, axis=1)
            rho_t = rho[e, sl, :]
            pull = None
            for p, (b_j, a_j, q_j) in enumerate(cols):
                g = lax.dot_general(x_t, b_j, (((1,), (1,)), ((), ())), preferred_element_type=jnp.float32)
                w = jnp.exp2(jnp.minimum(g * scale - a_t - a_j, 0.0)) * (q_t * q_j)
                if masked and p == t:
                    diag = lax.broadcasted_iota(jnp.int32, (TILE, TILE), 0) == lax.broadcasted_iota(jnp.int32, (TILE, TILE), 1)
                    w = jnp.where(diag, 0.0, w)
                for h in range(per):
                    rho_t = rho_t + w[:, h * LANES:(h + 1) * LANES]
                part = jnp.dot(w.astype(jnp.bfloat16), b_j, preferred_element_type=jnp.float32)
                pull = part if pull is None else pull + part
            pull = acc[e, sl, :] + pull
            if finish is None:
                rho[e, sl, :] = rho_t
                acc[e, sl, :] = pull
            else:
                finish(sl, force(e, sl, rho_t, pull))

    def force(e, sl, rho_t, pull):
        rho_sum = jnp.sum(rho_t, axis=1, keepdims=True)
        return (rho_sum * xg[e, me, sl, :].astype(jnp.float32) - pull) / feat

    barrier = pltpu.get_barrier_semaphore()
    for i in range(1, n):
        pl.semaphore_signal(barrier, inc=1, device_id={"blk": lax.rem(me + i, n)}, device_id_type=MESH)
    for k in range(tiles):
        load(k, 0).start()
        load(k, 1).start()
    q_load = pltpu.make_async_copy(q_hbm, q_ref, q_sem)
    q_load.start()
    acc[...] = jnp.zeros_like(acc)
    rho[...] = jnp.zeros_like(rho)
    for k in range(tiles):
        sl = tile_rows(k)
        load(k, 0).wait()
        load(k, 1).wait()
        x1 = xs[sl, :] + STEP * vs[sl, :]
        xg[1, me, sl, :] = x1.astype(jnp.bfloat16)
        xg[0, me, sl, :] = xs[sl, :].astype(jnp.bfloat16)
        if k == 0:
            pl.semaphore_wait(barrier, n - 1)
            for copy in own_copies(1, k):
                copy.start()
    q_load.wait()
    mg[me, 2] = q_ref[...]
    for k in range(tiles * per):
        sl = slice(k * LANES, (k + 1) * LANES)
        for e in (1, 0):
            b = xg[e, me, sl, :].astype(jnp.float32)
            s = jnp.sum(b * b, axis=1, keepdims=True) * (LOG2E / (2.0 * feat))
            wide = jnp.broadcast_to(s, (LANES, LANES))
            aw[e, sl, :] = wide
            mg[me, e, k:k + 1, :] = wide.T[0:1, :]
    for k in range(1, tiles):
        for copy in own_copies(1, k):
            copy.start()
        if k == 1:
            for copy in own_meta():
                copy.start()
    for k in range(tiles):
        for copy in own_copies(0, k):
            copy.start()
    for k in range(tiles * per):
        qw[k * LANES:(k + 1) * LANES, :] = jnp.broadcast_to(q_ref[k:k + 1, :], (LANES, LANES)).T

    @pl.loop(0, 2)
    def _(i):
        pair_tiles(1 - i, [(me, k) for k in range(tiles)], masked=True)

    meta_arrived(sib, SIB)

    @pl.loop(0, 2)
    def _(i):
        e = 1 - i
        for k in range(tiles):
            arrived(e, k, sib, SIB)
        pair_tiles(e, [(sib, k) for k in range(tiles)])

    def receive_sides(i):
        e, k = 1 - i // tiles, lax.rem(i, tiles)
        arrived(e, k, left, LEFT)
        fwd_left(e, k).start()

        @pl.when(k < half)
        def _():
            pass_right(e, k).start()

        arrived(e, k, right, RIGHT)
        fwd_right(e, k).start()

        @pl.when(k >= half)
        def _():
            pass_left(e, k).start()

    def own_sides(i):
        e, k = 1 - i // tiles, lax.rem(i, tiles)
        pair_tiles(e, [(left, k), (right, k)])

    def relayed_sides(i):
        e, k = 1 - i // tiles, lax.rem(i, tiles)
        arrived(e, k, left_sib, LEFT_SIB)
        arrived(e, k, right_sib, RIGHT_SIB)
        pair_tiles(e, [(left_sib, k), (right_sib, k)])

    def receive_opposite(e, k):
        for t in (k, k + half):
            arrived(e, t, opp, OPP)
            fwd_opp(e, t).start()

    def own_opposite(e, k):
        pair_tiles(e, [(opp, k), (opp, k + half)])

    def relayed_opposite(e, k, finish=None):
        for t in (k, k + half):
            arrived(e, t, opp_sib, OPP_SIB)
        pair_tiles(e, [(opp_sib, k), (opp_sib, k + half)], finish=finish)

    meta_arrived(left, LEFT)
    meta_arrived(right, RIGHT)
    for copy in fwd_meta():
        copy.start()
    meta_arrived(left_sib, LEFT_SIB)
    meta_arrived(right_sib, RIGHT_SIB)

    @pl.loop(0, 2 * tiles)
    def _(i):
        receive_sides(i)

        @pl.when(i > 0)
        def _():
            relayed_sides(i - 1)

        own_sides(i)

    meta_arrived(opp, OPP)
    fwd_opp_meta().start()
    receive_opposite(1, 0)
    relayed_sides(2 * tiles - 1)
    meta_arrived(opp_sib, OPP_SIB)

    def first_force(some):
        for t in some:
            sl = tile_rows(t)
            f1_ref[sl, :] = force(1, sl, rho[1, sl, :], acc[1, sl, :])

    @pl.loop(0, 2 * half - 1)
    def _(i):
        e, k = 1 - i // half, lax.rem(i, half)

        @pl.when(i > 0)
        def _():
            receive_opposite(e, k)

        own_opposite(e, k)

        @pl.when(i == half)
        def _():
            part = jnp.zeros((8, LANES), jnp.float32)
            for r in range(rows // 8):
                part = part + rho[1, r * 8:(r + 1) * 8, :]
            esend[...] = part
            ebuf[me] = part
            for p in range(1, n):
                energy_copy(p).start()
            first_force(range(half))

        relayed_opposite(e, k)

    last = half - 1
    receive_opposite(0, last)
    own_opposite(0, last)
    first_force(range(half, tiles))
    for i in range(1, n):
        energy_copy(i).wait_recv()
    total = ebuf[0]
    for b in range(1, n):
        total = total + ebuf[b]
    e_ref[...] = total

    def finish(sl, f0):
        v1 = vs[sl, :] + STEP * f0
        x2_ref[sl, :] = (xs[sl, :] + STEP * vs[sl, :]) + STEP * v1
        v2_ref[sl, :] = v1 + STEP * f1_ref[sl, :]

    relayed_opposite(0, last, finish=finish)

    for i in range(1, n):
        energy_copy(i).wait_send()
    for copy in own_meta() + fwd_meta() + (fwd_opp_meta(),):
        copy.wait_send()

    @pl.loop(0, 2 * tiles)
    def _(i):
        e = 1 - i // tiles
        k = lax.rem(i, tiles)
        for copy in own_copies(e, k) + (fwd_left(e, k), fwd_right(e, k), fwd_opp(e, k), pass_right(e, k)):
            copy.wait_send()


def write_out(f1_ref, x2_ref, v2_ref, parts_ref, f1_hbm, e_hbm, x2_hbm, v2_hbm, e_ref, sem):
    copies = [pltpu.make_async_copy(src, dst, sem.at[i])
              for i, (src, dst) in enumerate(((f1_ref, f1_hbm), (x2_ref, x2_hbm), (v2_ref, v2_hbm), (e_ref, e_hbm)))]
    for copy in copies[:3]:
        copy.start()
    e_ref[0] = 0.5 * jnp.sum(parts_ref[...])
    copies[3].start()
    for copy in copies:
        copy.wait()


def solution(mesh):
    n = mesh.shape["blk"]
    row_spec = P(("sys", "blk"), None)
    vec_spec = P(("sys", "blk"))

    def local_steps(positions, velocity, charges):
        rows, feat = positions.shape
        tiles = rows // TILE
        block = jax.ShapeDtypeStruct((rows, feat), jnp.float32)
        vmem = pl.BlockSpec(memory_space=pltpu.VMEM)
        hbm = pl.BlockSpec(memory_space=pltpu.HBM)
        dma = pltpu.SemaphoreType.DMA
        parts = pl.pallas_call(
            functools.partial(kernel, n),
            out_shape=(block, block, block, jax.ShapeDtypeStruct((8, LANES), jnp.float32)),
            in_specs=[hbm, hbm, hbm],
            out_specs=(vmem, vmem, vmem, vmem),
            scratch_shapes=[
                pltpu.VMEM((rows, feat), jnp.float32),
                pltpu.VMEM((rows, feat), jnp.float32),
                pltpu.VMEM((rows // LANES, LANES), jnp.float32),
                pltpu.VMEM((2, n, rows, feat), jnp.bfloat16),
                pltpu.VMEM((n, 3, rows // LANES, LANES), jnp.float32),
                pltpu.VMEM((2, rows, LANES), jnp.float32),
                pltpu.VMEM((rows, LANES), jnp.float32),
                pltpu.VMEM((2, rows, feat), jnp.float32),
                pltpu.VMEM((2, rows, LANES), jnp.float32),
                pltpu.VMEM((8, LANES), jnp.float32),
                pltpu.VMEM((n, 8, LANES), jnp.float32),
                dma((2, tiles)),
                dma,
                dma((3, 2, tiles)),
                dma((3,)),
                dma((4, 2, tiles)),
                dma((4,)),
                dma((7, 2, tiles)),
                dma((7,)),
                dma((n,)),
                dma((n,)),
            ],
            compiler_params=pltpu.CompilerParams(collective_id=0, has_side_effects=True, vmem_limit_bytes=52800000),
            cost_estimate=pl.CostEstimate(flops=8 * n * rows * rows * feat, bytes_accessed=20 * rows * feat, transcendentals=2 * n * rows * rows),
        )(*[pltpu.with_memory_space_constraint(x, pltpu.HBM) for x in (positions, velocity, charges.reshape(rows // LANES, LANES))])
        force_one, energy_one, pos_two, vel_two = pl.pallas_call(
            write_out,
            out_shape=(block, jax.ShapeDtypeStruct((1,), jnp.float32), block, block),
            in_specs=[vmem] * 4,
            out_specs=(hbm, hbm, hbm, hbm),
            scratch_shapes=[pltpu.SMEM((1,), jnp.float32), dma((4,))],
            compiler_params=pltpu.CompilerParams(vmem_limit_bytes=2**20),
        )(*parts)
        return force_one, energy_one, pos_two, vel_two

    return jax.shard_map(local_steps, mesh=mesh, in_specs=(row_spec, row_spec, vec_spec), out_specs=(row_spec, P("sys"), row_spec, row_spec), check_vma=False)
```

```python
import functools
import math

import jax
import jax.numpy as jnp
from jax import lax
from jax.experimental import pallas as pl
from jax.experimental.pallas import tpu as pltpu
from jax.sharding import PartitionSpec as P

MESH = pl.DeviceIdType.MESH
STEP = 0.5
LOG2E = math.log2(math.e)
TILE = 256
LANES = 128
SIB, LEFT, RIGHT, LEFT_SIB, RIGHT_SIB, OPP, OPP_SIB = range(7)


def kernel(n, x0_hbm, v0_hbm, q_hbm, f1_ref, x2_ref, v2_ref, e_ref,
           xs, vs, q_ref, xg, mg, aw, qw, acc, rho, esend, ebuf,
           load_sem, q_sem, own_send, own_meta_send, fwd_send, fwd_meta_send, recv_sem, meta_recv, e_send, e_recv):
    rows, feat = xs.shape
    tiles = rows // TILE
    per = TILE // LANES
    half = tiles // 2
    me = lax.axis_index("blk")
    core = lax.rem(me, 2)
    sib = me + 1 - 2 * core
    right = lax.rem(me + 2, n)
    left = lax.rem(me + n - 2, n)
    opp = lax.rem(me + n // 2, n)
    left_sib = left + 1 - 2 * core
    right_sib = right + 1 - 2 * core
    opp_sib = opp + 1 - 2 * core

    def tile_rows(k):
        return pl.ds(k * TILE, TILE) if isinstance(k, int) else pl.ds(pl.multiple_of(k * TILE, TILE), TILE)

    def block_copy(e, k, blk, dev, send, rel):
        ref = xg.at[e, blk, tile_rows(k), :]
        return pltpu.make_async_remote_copy(src_ref=ref, dst_ref=ref, send_sem=send, recv_sem=recv_sem.at[rel, e, k],
                                            device_id={"blk": dev}, device_id_type=MESH)

    def meta_copy(blk, dev, send, rel):
        ref = mg.at[blk]
        return pltpu.make_async_remote_copy(src_ref=ref, dst_ref=ref, send_sem=send, recv_sem=meta_recv.at[rel],
                                            device_id={"blk": dev}, device_id_type=MESH)

    def own_copies(e, k):
        return (block_copy(e, k, me, right, own_send.at[0, e, k], LEFT),
                block_copy(e, k, me, left, own_send.at[1, e, k], RIGHT),
                block_copy(e, k, me, sib, own_send.at[2, e, k], SIB))

    def own_meta():
        return (meta_copy(me, right, own_meta_send.at[0], LEFT),
                meta_copy(me, left, own_meta_send.at[1], RIGHT),
                meta_copy(me, sib, own_meta_send.at[2], SIB))

    def fwd_left(e, k):
        return block_copy(e, k, left, sib, fwd_send.at[0, e, k], LEFT_SIB)

    def fwd_right(e, k):
        return block_copy(e, k, right, sib, fwd_send.at[1, e, k], RIGHT_SIB)

    def fwd_opp(e, k):
        return block_copy(e, k, opp, sib, fwd_send.at[2, e, k], OPP_SIB)

    def pass_right(e, k):
        return block_copy(e, k, left, right, fwd_send.at[3, e, k], OPP)

    def pass_left(e, k):
        return block_copy(e, k, right, left, fwd_send.at[3, e, k], OPP)

    def fwd_meta():
        return (meta_copy(left, sib, fwd_meta_send.at[0], LEFT_SIB),
                meta_copy(right, sib, fwd_meta_send.at[1], RIGHT_SIB),
                meta_copy(left, right, fwd_meta_send.at[2], OPP))

    def fwd_opp_meta():
        return meta_copy(opp, sib, fwd_meta_send.at[3], OPP_SIB)

    def arrived(e, k, blk, rel):
        block_copy(e, k, blk, sib, own_send.at[0, e, k], rel).wait_recv()

    def meta_arrived(blk, rel):
        meta_copy(blk, sib, own_meta_send.at[0], rel).wait_recv()

    def energy_copy(i):
        return pltpu.make_async_remote_copy(src_ref=esend, dst_ref=ebuf.at[me], send_sem=e_send.at[i], recv_sem=e_recv.at[i],
                                            device_id={"blk": lax.rem(me + i, n)}, device_id_type=MESH)

    def load(k, which):
        src, dst = ((x0_hbm, xs), (v0_hbm, vs))[which]
        return pltpu.make_async_copy(src.at[tile_rows(k), :], dst.at[tile_rows(k), :], load_sem.at[which, k])

    def pair_tiles(e, pieces, masked=False, finish=None):
        scale = LOG2E / feat
        cols = []
        for blk, k in pieces:
            b_j = xg[e, blk, tile_rows(k), :]
            a_j = jnp.concatenate([mg[blk, e, pl.ds(k * per + p, 1), :] for p in range(per)], axis=1)
            q_j = jnp.concatenate([mg[blk, 2, pl.ds(k * per + p, 1), :] for p in range(per)], axis=1)
            cols.append((b_j, a_j, q_j))
        for t in range(tiles):
            sl = tile_rows(t)
            x_t = xg[e, me, sl, :]
            a_t = jnp.concatenate([aw[e, sl, :]] * per, axis=1)
            q_t = jnp.concatenate([qw[sl, :]] * per, axis=1)
            rho_t = rho[e, sl, :]
            pull = None
            for p, (b_j, a_j, q_j) in enumerate(cols):
                g = lax.dot_general(x_t, b_j, (((1,), (1,)), ((), ())), preferred_element_type=jnp.float32)
                w = jnp.exp2(jnp.minimum(g * scale - a_t - a_j, 0.0)) * (q_t * q_j)
                if masked and p == t:
                    diag = lax.broadcasted_iota(jnp.int32, (TILE, TILE), 0) == lax.broadcasted_iota(jnp.int32, (TILE, TILE), 1)
                    w = jnp.where(diag, 0.0, w)
                for h in range(per):
                    rho_t = rho_t + w[:, h * LANES:(h + 1) * LANES]
                part = jnp.dot(w.astype(jnp.bfloat16), b_j, preferred_element_type=jnp.float32)
                pull = part if pull is None else pull + part
            pull = acc[e, sl, :] + pull
            rho[e, sl, :] = rho_t
            if finish is None:
                acc[e, sl, :] = pull
            else:
                finish(sl, force(e, sl, rho_t, pull))

    def force(e, sl, rho_t, pull):
        rho_sum = jnp.sum(rho_t, axis=1, keepdims=True)
        return (rho_sum * xg[e, me, sl, :].astype(jnp.float32) - pull) / feat

    barrier = pltpu.get_barrier_semaphore()
    for i in range(1, n):
        pl.semaphore_signal(barrier, inc=1, device_id={"blk": lax.rem(me + i, n)}, device_id_type=MESH)
    load(0, 0).start()
    load(0, 1).start()
    q_load = pltpu.make_async_copy(q_hbm, q_ref, q_sem)
    rho[...] = jnp.zeros_like(rho)
    for k in range(1, tiles):
        load(k, 0).start()
        load(k, 1).start()
    q_load.start()
    acc[...] = jnp.zeros_like(acc)
    for k in range(tiles):
        sl = tile_rows(k)
        load(k, 0).wait()
        load(k, 1).wait()
        x1 = xs[sl, :] + STEP * vs[sl, :]
        xg[1, me, sl, :] = x1.astype(jnp.bfloat16)
        xg[0, me, sl, :] = xs[sl, :].astype(jnp.bfloat16)
        if k == 0:
            pl.semaphore_wait(barrier, n - 1)
            for copy in own_copies(1, k):
                copy.start()
    q_load.wait()
    mg[me, 2] = q_ref[...]
    for k in range(tiles * per):
        sl = slice(k * LANES, (k + 1) * LANES)
        for e in (1, 0):
            b = xg[e, me, sl, :].astype(jnp.float32)
            s = jnp.sum(b * b, axis=1, keepdims=True) * (LOG2E / (2.0 * feat))
            wide = jnp.broadcast_to(s, (LANES, LANES))
            aw[e, sl, :] = wide
            mg[me, e, k:k + 1, :] = wide.T[0:1, :]
    for k in range(1, tiles):
        for copy in own_copies(1, k):
            copy.start()
        if k == 1:
            for copy in own_meta():
                copy.start()
    for k in range(tiles):
        for copy in own_copies(0, k):
            copy.start()
    for k in range(tiles * per):
        qw[k * LANES:(k + 1) * LANES, :] = jnp.broadcast_to(q_ref[k:k + 1, :], (LANES, LANES)).T

    @pl.loop(0, 2)
    def _(i):
        pair_tiles(1 - i, [(me, k) for k in range(tiles)], masked=True)

    meta_arrived(sib, SIB)

    @pl.loop(0, 2)
    def _(i):
        e = 1 - i
        for k in range(tiles):
            arrived(e, k, sib, SIB)
        pair_tiles(e, [(sib, k) for k in range(tiles)])

    def receive_sides(i):
        e, k = 1 - i // tiles, lax.rem(i, tiles)
        arrived(e, k, left, LEFT)
        fwd_left(e, k).start()

        @pl.when(k < half)
        def _():
            pass_right(e, k).start()

        arrived(e, k, right, RIGHT)
        fwd_right(e, k).start()

        @pl.when(k >= half)
        def _():
            pass_left(e, k).start()

    def relayed_sides(e, k):
        arrived(e, k, left_sib, LEFT_SIB)
        arrived(e, k, right_sib, RIGHT_SIB)
        return [(left_sib, k), (right_sib, k)]

    def receive_opposite(e, k):
        for t in (k, k + half):
            arrived(e, t, opp, OPP)
            fwd_opp(e, t).start()

    def relayed_opposite(e, k):
        for t in (k, k + half):
            arrived(e, t, opp_sib, OPP_SIB)
        return [(opp_sib, k), (opp_sib, k + half)]

    meta_arrived(left, LEFT)
    meta_arrived(right, RIGHT)
    for copy in fwd_meta():
        copy.start()
    meta_arrived(left_sib, LEFT_SIB)
    meta_arrived(right_sib, RIGHT_SIB)

    @pl.loop(0, 2 * tiles)
    def _(i):
        e, k = 1 - i // tiles, lax.rem(i, tiles)
        receive_sides(i)
        sides = [(left, k), (right, k)]

        @pl.when(k > 0)
        def _():
            pair_tiles(e, sides + relayed_sides(e, k - 1))

        @pl.when(k == 0)
        def _():
            @pl.when(i > 0)
            def _():
                pair_tiles(1, relayed_sides(1, tiles - 1))

            pair_tiles(e, sides)

    def first_finish(sl, f1):
        f1_ref[sl, :] = f1

    def last_finish(sl, f0):
        v1 = vs[sl, :] + STEP * f0
        x2_ref[sl, :] = (xs[sl, :] + STEP * vs[sl, :]) + STEP * v1
        v2_ref[sl, :] = v1 + STEP * f1_ref[sl, :]

    meta_arrived(opp, OPP)
    fwd_opp_meta().start()
    receive_opposite(1, 0)
    pair_tiles(0, relayed_sides(0, tiles - 1))
    meta_arrived(opp_sib, OPP_SIB)

    @pl.loop(0, 2)
    def _(i):
        e = 1 - i

        @pl.when(i == 1)
        def _():
            pair_tiles(1, relayed_opposite(1, half - 1), finish=first_finish)
            part = jnp.zeros((8, LANES), jnp.float32)
            for r in range(rows // 8):
                part = part + rho[1, r * 8:(r + 1) * 8, :]
            esend[...] = part
            ebuf[me] = part
            for p in range(1, n):
                energy_copy(p).start()
            receive_opposite(0, 0)

        pair_tiles(e, [(opp, 0), (opp, half)])
        for k in range(1, half):
            receive_opposite(e, k)
            pair_tiles(e, [(opp, k), (opp, k + half)] + relayed_opposite(e, k - 1))

    pair_tiles(0, relayed_opposite(0, half - 1), finish=last_finish)
    for i in range(1, n):
        energy_copy(i).wait_recv()
    e_ref[...] = ebuf[...]

    for i in range(1, n):
        energy_copy(i).wait_send()
    for copy in own_meta() + fwd_meta() + (fwd_opp_meta(),):
        copy.wait_send()

    @pl.loop(0, 2 * tiles)
    def _(i):
        e = 1 - i // tiles
        k = lax.rem(i, tiles)
        for copy in own_copies(e, k) + (fwd_left(e, k), fwd_right(e, k), fwd_opp(e, k), pass_right(e, k)):
            copy.wait_send()


def write_out(f1_ref, x2_ref, v2_ref, parts_ref, f1_hbm, e_hbm, x2_hbm, v2_hbm, e_ref, sem):
    copies = [pltpu.make_async_copy(src, dst, sem.at[i])
              for i, (src, dst) in enumerate(((f1_ref, f1_hbm), (x2_ref, x2_hbm), (v2_ref, v2_hbm), (e_ref, e_hbm)))]
    for copy in copies[:3]:
        copy.start()
    total = parts_ref[0]
    for b in range(1, parts_ref.shape[0]):
        total = total + parts_ref[b]
    e_ref[0] = 0.5 * jnp.sum(total)
    copies[3].start()
    for copy in copies:
        copy.wait()


def solution(mesh):
    n = mesh.shape["blk"]
    row_spec = P(("sys", "blk"), None)
    vec_spec = P(("sys", "blk"))

    def local_steps(positions, velocity, charges):
        rows, feat = positions.shape
        tiles = rows // TILE
        block = jax.ShapeDtypeStruct((rows, feat), jnp.float32)
        vmem = pl.BlockSpec(memory_space=pltpu.VMEM)
        hbm = pl.BlockSpec(memory_space=pltpu.HBM)
        dma = pltpu.SemaphoreType.DMA
        parts = pl.pallas_call(
            functools.partial(kernel, n),
            out_shape=(block, block, block, jax.ShapeDtypeStruct((n, 8, LANES), jnp.float32)),
            in_specs=[hbm, hbm, hbm],
            out_specs=(vmem, vmem, vmem, vmem),
            scratch_shapes=[
                pltpu.VMEM((rows, feat), jnp.float32),
                pltpu.VMEM((rows, feat), jnp.float32),
                pltpu.VMEM((rows // LANES, LANES), jnp.float32),
                pltpu.VMEM((2, n, rows, feat), jnp.bfloat16),
                pltpu.VMEM((n, 3, rows // LANES, LANES), jnp.float32),
                pltpu.VMEM((2, rows, LANES), jnp.float32),
                pltpu.VMEM((rows, LANES), jnp.float32),
                pltpu.VMEM((2, rows, feat), jnp.float32),
                pltpu.VMEM((2, rows, LANES), jnp.float32),
                pltpu.VMEM((8, LANES), jnp.float32),
                pltpu.VMEM((n, 8, LANES), jnp.float32),
                dma((2, tiles)),
                dma,
                dma((3, 2, tiles)),
                dma((3,)),
                dma((4, 2, tiles)),
                dma((4,)),
                dma((7, 2, tiles)),
                dma((7,)),
                dma((n,)),
                dma((n,)),
            ],
            compiler_params=pltpu.CompilerParams(collective_id=0, has_side_effects=True, vmem_limit_bytes=52800000),
            cost_estimate=pl.CostEstimate(flops=8 * n * rows * rows * feat, bytes_accessed=20 * rows * feat, transcendentals=2 * n * rows * rows),
        )(*[pltpu.with_memory_space_constraint(x, pltpu.HBM) for x in (positions, velocity, charges.reshape(rows // LANES, LANES))])
        force_one, energy_one, pos_two, vel_two = pl.pallas_call(
            write_out,
            out_shape=(block, jax.ShapeDtypeStruct((1,), jnp.float32), block, block),
            in_specs=[vmem] * 4,
            out_specs=(hbm, hbm, hbm, hbm),
            scratch_shapes=[pltpu.SMEM((1,), jnp.float32), dma((4,))],
            compiler_params=pltpu.CompilerParams(vmem_limit_bytes=2**20),
        )(*parts)
        return force_one, energy_one, pos_two, vel_two

    return jax.shard_map(local_steps, mesh=mesh, in_specs=(row_spec, row_spec, vec_spec), out_specs=(row_spec, P("sys"), row_spec, row_spec), check_vma=False)
```

```python
import functools
import math

import jax
import jax.numpy as jnp
from jax import lax
from jax.experimental import pallas as pl
from jax.experimental.pallas import tpu as pltpu
from jax.sharding import PartitionSpec as P

MESH = pl.DeviceIdType.MESH
STEP = 0.5
LOG2E = math.log2(math.e)
TILE = 256
LANES = 128
SIB, SIDES, SIDES_SIB, OPP, OPP_SIB = range(5)


def kernel(n, x0_hbm, v0_hbm, q_hbm, f1_ref, x2_ref, v2_ref, e_ref,
           xs, vs, q_ref, xg, mg, aw, qw, acc, rho, esend, ebuf,
           load_sem, q_sem, sent, meta_sent, e_sent, meta_recv, e_recv, sib_recv, side_recv, side_sib_recv, opp_recv, opp_sib_recv):
    rows, feat = xs.shape
    tiles = rows // TILE
    per = TILE // LANES
    half = tiles // 2
    me = lax.axis_index("blk")
    core = lax.rem(me, 2)
    sib = me + 1 - 2 * core
    right = lax.rem(me + 2, n)
    left = lax.rem(me + n - 2, n)
    opp = lax.rem(me + n // 2, n)
    left_sib = left + 1 - 2 * core
    right_sib = right + 1 - 2 * core
    opp_sib = opp + 1 - 2 * core

    def tile_rows(k):
        return pl.ds(k * TILE, TILE) if isinstance(k, int) else pl.ds(pl.multiple_of(k * TILE, TILE), TILE)

    def remote(ref, dev, send, recv):
        return pltpu.make_async_remote_copy(src_ref=ref, dst_ref=ref, send_sem=send, recv_sem=recv,
                                            device_id={"blk": dev}, device_id_type=MESH)

    def block_copy(e, k, blk, dev, recv):
        return remote(xg.at[e, blk, tile_rows(k), :], dev, sent, recv)

    def meta_copy(blk, dev, rel):
        return remote(mg.at[blk], dev, meta_sent, meta_recv.at[rel])

    def own_copies(e, k):
        return (block_copy(e, k, me, right, side_recv.at[e, k]),
                block_copy(e, k, me, left, side_recv.at[e, k]),
                block_copy(e, k, me, sib, sib_recv.at[e]))

    def own_meta():
        return (meta_copy(me, right, SIDES), meta_copy(me, left, SIDES), meta_copy(me, sib, SIB))

    def fwd_left(e, k):
        return block_copy(e, k, left, sib, side_sib_recv.at[e, k])

    def fwd_right(e, k):
        return block_copy(e, k, right, sib, side_sib_recv.at[e, k])

    def fwd_opp(e, k):
        return block_copy(e, k, opp, sib, opp_sib_recv.at[e, lax.rem(k, half)])

    def pass_right(e, k):
        return block_copy(e, k, left, right, opp_recv.at[e, k])

    def pass_left(e, k):
        return block_copy(e, k, right, left, opp_recv.at[e, k - half])

    def fwd_meta():
        return (meta_copy(left, sib, SIDES_SIB), meta_copy(right, sib, SIDES_SIB), meta_copy(left, right, OPP))

    def fwd_opp_meta():
        return meta_copy(opp, sib, OPP_SIB)

    def tiles_arrived(count, recv):
        remote(xg.at[0, 0, pl.ds(0, count * TILE), :], sib, sent, recv).wait_recv()

    def meta_arrived(count, rel):
        remote(mg.at[pl.ds(0, count)], sib, meta_sent, meta_recv.at[rel]).wait_recv()

    def energy_copy(i):
        return pltpu.make_async_remote_copy(src_ref=esend, dst_ref=ebuf.at[me], send_sem=e_sent, recv_sem=e_recv,
                                            device_id={"blk": lax.rem(me + i, n)}, device_id_type=MESH)

    def load(which, lo, size):
        src, dst = ((x0_hbm, xs), (v0_hbm, vs))[which]
        part = pl.ds(lo, size)
        return pltpu.make_async_copy(src.at[part, :], dst.at[part, :], load_sem.at[which, 1 if lo else 0])

    def pair_tiles(e, pieces, masked=False, finish=None):
        scale = LOG2E / feat
        cols = []
        for blk, k in pieces:
            b_j = xg[e, blk, tile_rows(k), :]
            a_j = jnp.concatenate([mg[blk, e, pl.ds(k * per + p, 1), :] for p in range(per)], axis=1)
            q_j = jnp.concatenate([mg[blk, 2, pl.ds(k * per + p, 1), :] for p in range(per)], axis=1)
            cols.append((b_j, a_j, q_j))
        for t in range(tiles):
            sl = tile_rows(t)
            x_t = xg[e, me, sl, :]
            a_t = jnp.concatenate([aw[e, sl, :]] * per, axis=1)
            q_t = jnp.concatenate([qw[sl, :]] * per, axis=1)
            rho_t = rho[e, sl, :]
            pull = None
            for p, (b_j, a_j, q_j) in enumerate(cols):
                g = lax.dot_general(x_t, b_j, (((1,), (1,)), ((), ())), preferred_element_type=jnp.float32)
                w = jnp.exp2(jnp.minimum(g * scale - a_t - a_j, 0.0)) * (q_t * q_j)
                if masked and p == t:
                    diag = lax.broadcasted_iota(jnp.int32, (TILE, TILE), 0) == lax.broadcasted_iota(jnp.int32, (TILE, TILE), 1)
                    w = jnp.where(diag, 0.0, w)
                for h in range(per):
                    rho_t = rho_t + w[:, h * LANES:(h + 1) * LANES]
                part = jnp.dot(w.astype(jnp.bfloat16), b_j, preferred_element_type=jnp.float32)
                pull = part if pull is None else pull + part
            pull = acc[e, sl, :] + pull
            rho[e, sl, :] = rho_t
            if finish is None:
                acc[e, sl, :] = pull
            else:
                finish(sl, force(e, sl, rho_t, pull))

    def force(e, sl, rho_t, pull):
        rho_sum = jnp.sum(rho_t, axis=1, keepdims=True)
        return (rho_sum * xg[e, me, sl, :].astype(jnp.float32) - pull) / feat

    barrier = pltpu.get_barrier_semaphore()
    for i in range(1, n):
        pl.semaphore_signal(barrier, inc=1, device_id={"blk": lax.rem(me + i, n)}, device_id_type=MESH)
    first = [load(which, 0, TILE) for which in range(2)]
    others = [load(which, TILE, rows - TILE) for which in range(2)]
    for copy in first:
        copy.start()
    q_load = pltpu.make_async_copy(q_hbm, q_ref, q_sem)
    rho[...] = jnp.zeros_like(rho)
    for copy in others:
        copy.start()
    q_load.start()
    acc[...] = jnp.zeros_like(acc)
    for k in range(tiles):
        sl = tile_rows(k)
        if k < 2:
            for copy in (first, others)[k]:
                copy.wait()
        x0 = xs[sl, :]
        x1 = x0 + STEP * vs[sl, :]
        xg[1, me, sl, :] = x1.astype(jnp.bfloat16)
        xg[0, me, sl, :] = x0.astype(jnp.bfloat16)
        xs[sl, :] = x1
        if k == 0:
            pl.semaphore_wait(barrier, n - 1)
            for copy in own_copies(1, k):
                copy.start()
    q_load.wait()
    mg[me, 2] = q_ref[...]
    for k in range(tiles * per):
        sl = slice(k * LANES, (k + 1) * LANES)
        for e in (1, 0):
            b = xg[e, me, sl, :].astype(jnp.float32)
            s = jnp.sum(b * b, axis=1, keepdims=True) * (LOG2E / (2.0 * feat))
            wide = jnp.broadcast_to(s, (LANES, LANES))
            aw[e, sl, :] = wide
            mg[me, e, k:k + 1, :] = wide.T[0:1, :]
    for k in range(1, tiles):
        for copy in own_copies(1, k):
            copy.start()
        if k == 1:
            for copy in own_meta():
                copy.start()
    for k in range(tiles):
        for copy in own_copies(0, k):
            copy.start()
    for k in range(tiles * per):
        qw[k * LANES:(k + 1) * LANES, :] = jnp.broadcast_to(q_ref[k:k + 1, :], (LANES, LANES)).T

    @pl.loop(0, 2)
    def _(i):
        pair_tiles(1 - i, [(me, k) for k in range(tiles)], masked=True)

    meta_arrived(1, SIB)

    @pl.loop(0, 2)
    def _(i):
        e = 1 - i
        tiles_arrived(tiles, sib_recv.at[e])
        pair_tiles(e, [(sib, k) for k in range(tiles)])

    def receive_sides(i):
        e, k = 1 - i // tiles, lax.rem(i, tiles)
        tiles_arrived(2, side_recv.at[e, k])
        fwd_left(e, k).start()
        fwd_right(e, k).start()

        @pl.when(k < half)
        def _():
            pass_right(e, k).start()

        @pl.when(k >= half)
        def _():
            pass_left(e, k).start()

    def relayed_sides(e, k):
        tiles_arrived(2, side_sib_recv.at[e, k])
        return [(left_sib, k), (right_sib, k)]

    def receive_opposite(e, k):
        tiles_arrived(2, opp_recv.at[e, k])
        for t in (k, k + half):
            fwd_opp(e, t).start()

    def relayed_opposite(e, k):
        tiles_arrived(2, opp_sib_recv.at[e, k])
        return [(opp_sib, k), (opp_sib, k + half)]

    meta_arrived(2, SIDES)
    for copy in fwd_meta():
        copy.start()
    meta_arrived(2, SIDES_SIB)

    @pl.loop(0, 2 * tiles)
    def _(i):
        e, k = 1 - i // tiles, lax.rem(i, tiles)
        receive_sides(i)
        sides = [(left, k), (right, k)]

        @pl.when(k > 0)
        def _():
            pair_tiles(e, sides + relayed_sides(e, k - 1))

        @pl.when(k == 0)
        def _():
            @pl.when(i > 0)
            def _():
                pair_tiles(1, relayed_sides(1, tiles - 1))

            pair_tiles(e, sides)

    def first_finish(sl, f1):
        f1_ref[sl, :] = f1

    def last_finish(sl, f0):
        v1 = vs[sl, :] + STEP * f0
        x2_ref[sl, :] = xs[sl, :] + STEP * v1
        v2_ref[sl, :] = v1 + STEP * f1_ref[sl, :]

    meta_arrived(1, OPP)
    fwd_opp_meta().start()
    receive_opposite(1, 0)
    pair_tiles(0, relayed_sides(0, tiles - 1))
    meta_arrived(1, OPP_SIB)

    @pl.loop(0, 2)
    def _(i):
        e = 1 - i

        @pl.when(i == 1)
        def _():
            pair_tiles(1, relayed_opposite(1, half - 1), finish=first_finish)
            part = jnp.zeros((8, LANES), jnp.float32)
            for r in range(rows // 8):
                part = part + rho[1, r * 8:(r + 1) * 8, :]
            esend[...] = part
            ebuf[me] = part
            for p in range(1, n):
                energy_copy(p).start()
            receive_opposite(0, 0)

        pair_tiles(e, [(opp, 0), (opp, half)])
        for k in range(1, half):
            receive_opposite(e, k)
            pair_tiles(e, [(opp, k), (opp, k + half)] + relayed_opposite(e, k - 1))

    pair_tiles(0, relayed_opposite(0, half - 1), finish=last_finish)
    parts = remote(ebuf.at[pl.ds(0, n - 1)], sib, e_sent, e_recv)
    parts.wait_recv()
    e_ref[...] = ebuf[...]
    parts.wait_send()
    remote(xg.at[:, pl.ds(0, n - 1)], sib, sent, sib_recv.at[0]).wait_send()
    remote(mg.at[pl.ds(0, n - 1)], sib, meta_sent, meta_recv.at[0]).wait_send()


def write_out(f1_ref, x2_ref, v2_ref, parts_ref, f1_hbm, e_hbm, x2_hbm, v2_hbm, e_ref, sem):
    copies = [pltpu.make_async_copy(src, dst, sem.at[i])
              for i, (src, dst) in enumerate(((f1_ref, f1_hbm), (x2_ref, x2_hbm), (v2_ref, v2_hbm), (e_ref, e_hbm)))]
    for copy in copies[:3]:
        copy.start()
    total = parts_ref[0]
    for b in range(1, parts_ref.shape[0]):
        total = total + parts_ref[b]
    e_ref[0] = 0.5 * jnp.sum(total)
    copies[3].start()
    for copy in copies:
        copy.wait()


def solution(mesh):
    n = mesh.shape["blk"]
    row_spec = P(("sys", "blk"), None)
    vec_spec = P(("sys", "blk"))

    def local_steps(positions, velocity, charges):
        rows, feat = positions.shape
        tiles = rows // TILE
        block = jax.ShapeDtypeStruct((rows, feat), jnp.float32)
        vmem = pl.BlockSpec(memory_space=pltpu.VMEM)
        hbm = pl.BlockSpec(memory_space=pltpu.HBM)
        dma = pltpu.SemaphoreType.DMA
        parts = pl.pallas_call(
            functools.partial(kernel, n),
            out_shape=(block, block, block, jax.ShapeDtypeStruct((n, 8, LANES), jnp.float32)),
            in_specs=[hbm, hbm, hbm],
            out_specs=(vmem, vmem, vmem, vmem),
            scratch_shapes=[
                pltpu.VMEM((rows, feat), jnp.float32),
                pltpu.VMEM((rows, feat), jnp.float32),
                pltpu.VMEM((rows // LANES, LANES), jnp.float32),
                pltpu.VMEM((2, n, rows, feat), jnp.bfloat16),
                pltpu.VMEM((n, 3, rows // LANES, LANES), jnp.float32),
                pltpu.VMEM((2, rows, LANES), jnp.float32),
                pltpu.VMEM((rows, LANES), jnp.float32),
                pltpu.VMEM((2, rows, feat), jnp.float32),
                pltpu.VMEM((2, rows, LANES), jnp.float32),
                pltpu.VMEM((8, LANES), jnp.float32),
                pltpu.VMEM((n, 8, LANES), jnp.float32),
                dma((2, 2)),
                dma,
                dma,
                dma,
                dma,
                dma((5,)),
                dma,
                dma((2,)),
                dma((2, tiles)),
                dma((2, tiles)),
                dma((2, tiles // 2)),
                dma((2, tiles // 2)),
            ],
            compiler_params=pltpu.CompilerParams(collective_id=0, has_side_effects=True, vmem_limit_bytes=52800000),
            cost_estimate=pl.CostEstimate(flops=8 * n * rows * rows * feat, bytes_accessed=20 * rows * feat, transcendentals=2 * n * rows * rows),
        )(*[pltpu.with_memory_space_constraint(x, pltpu.HBM) for x in (positions, velocity, charges.reshape(rows // LANES, LANES))])
        force_one, energy_one, pos_two, vel_two = pl.pallas_call(
            write_out,
            out_shape=(block, jax.ShapeDtypeStruct((1,), jnp.float32), block, block),
            in_specs=[vmem] * 4,
            out_specs=(hbm, hbm, hbm, hbm),
            scratch_shapes=[pltpu.SMEM((1,), jnp.float32), dma((4,))],
            compiler_params=pltpu.CompilerParams(vmem_limit_bytes=2**20),
        )(*parts)
        return force_one, energy_one, pos_two, vel_two

    return jax.shard_map(local_steps, mesh=mesh, in_specs=(row_spec, row_spec, vec_spec), out_specs=(row_spec, P("sys"), row_spec, row_spec), check_vma=False)
```

```python
import functools
import math

import jax
import jax.numpy as jnp
from jax import lax
from jax.experimental import pallas as pl
from jax.experimental.pallas import tpu as pltpu
from jax.sharding import PartitionSpec as P

MESH = pl.DeviceIdType.MESH
STEP = 0.5
LOG2E = math.log2(math.e)
TILE = 256
LANES = 128
SIB, SIDES, SIDES_SIB, OPP, OPP_SIB = range(5)


def kernel(n, x0_hbm, v0_hbm, q_hbm, f1_ref, x2_ref, v2_ref, e_ref,
           xs, vs, q_ref, xg, mg, aw, qw, acc, rho, esend, ebuf,
           load_sem, q_sem, sent, meta_sent, e_sent, meta_recv, e_recv, sib_recv, side_recv, side_sib_recv, opp_recv, opp_sib_recv):
    rows, feat = xs.shape
    tiles = rows // TILE
    per = TILE // LANES
    half = tiles // 2
    strips = half * per
    me = lax.axis_index("blk")
    core = lax.rem(me, 2)
    sib = me + 1 - 2 * core
    right = lax.rem(me + 2, n)
    left = lax.rem(me + n - 2, n)
    opp = lax.rem(me + n // 2, n)
    left_sib = left + 1 - 2 * core
    right_sib = right + 1 - 2 * core
    opp_sib = opp + 1 - 2 * core

    def tile_rows(k):
        return pl.ds(k * TILE, TILE) if isinstance(k, int) else pl.ds(pl.multiple_of(k * TILE, TILE), TILE)

    def remote(ref, dev, send, recv):
        return pltpu.make_async_remote_copy(src_ref=ref, dst_ref=ref, send_sem=send, recv_sem=recv,
                                            device_id={"blk": dev}, device_id_type=MESH)

    def strip_rows(r):
        return pl.ds(r * LANES, LANES) if isinstance(r, int) else pl.ds(pl.multiple_of(r * LANES, LANES), LANES)

    def tile(blk, k):
        return blk, [k * per + p for p in range(per)]

    def opposite_strips(s):
        return s, s + strips

    def opposite_piece(blk, s):
        return blk, opposite_strips(s)

    def strip_copy(e, r, blk, dev, recv):
        return remote(xg.at[e, blk, strip_rows(r), :], dev, sent, recv)

    def block_copy(e, k, blk, dev, recv):
        return remote(xg.at[e, blk, tile_rows(k), :], dev, sent, recv)

    def meta_copy(blk, dev, rel):
        return remote(mg.at[blk], dev, meta_sent, meta_recv.at[rel])

    def own_copies(e, k):
        return (block_copy(e, k, me, right, side_recv.at[e, k]),
                block_copy(e, k, me, left, side_recv.at[e, k]),
                block_copy(e, k, me, sib, sib_recv.at[e]))

    def own_meta():
        return (meta_copy(me, right, SIDES), meta_copy(me, left, SIDES), meta_copy(me, sib, SIB))

    def fwd_left(e, k):
        return block_copy(e, k, left, sib, side_sib_recv.at[e, k])

    def fwd_right(e, k):
        return block_copy(e, k, right, sib, side_sib_recv.at[e, k])

    def pass_right(e, k):
        return [strip_copy(e, k * per + p, left, right, opp_recv.at[e, k * per + p]) for p in range(per)]

    def pass_left(e, k):
        return [strip_copy(e, k * per + p, right, left, opp_recv.at[e, k * per + p - strips]) for p in range(per)]

    def fwd_meta():
        return (meta_copy(left, sib, SIDES_SIB), meta_copy(right, sib, SIDES_SIB), meta_copy(left, right, OPP))

    def fwd_opp_meta():
        return meta_copy(opp, sib, OPP_SIB)

    def tiles_arrived(count, recv):
        remote(xg.at[0, 0, pl.ds(0, count * TILE), :], sib, sent, recv).wait_recv()

    def meta_arrived(count, rel):
        remote(mg.at[pl.ds(0, count)], sib, meta_sent, meta_recv.at[rel]).wait_recv()

    def energy_copy(i):
        return pltpu.make_async_remote_copy(src_ref=esend, dst_ref=ebuf.at[me], send_sem=e_sent, recv_sem=e_recv,
                                            device_id={"blk": lax.rem(me + i, n)}, device_id_type=MESH)

    def load(which, lo, size):
        src, dst = ((x0_hbm, xs), (v0_hbm, vs))[which]
        part = pl.ds(lo, size)
        return pltpu.make_async_copy(src.at[part, :], dst.at[part, :], load_sem.at[which, 1 if lo else 0])

    def pair_tiles(e, pieces, masked=False, finish=None):
        scale = LOG2E / feat
        cols = []
        for blk, strips in pieces:
            b_j = jnp.concatenate([xg[e, blk, strip_rows(r), :] for r in strips], axis=0)
            a_j = jnp.concatenate([mg[blk, e, pl.ds(r, 1), :] for r in strips], axis=1)
            q_j = jnp.concatenate([mg[blk, 2, pl.ds(r, 1), :] for r in strips], axis=1)
            cols.append((b_j, a_j, q_j))
        for t in range(tiles):
            sl = tile_rows(t)
            x_t = xg[e, me, sl, :]
            a_t = jnp.concatenate([aw[e, sl, :]] * per, axis=1)
            q_t = jnp.concatenate([qw[sl, :]] * per, axis=1)
            rho_t = rho[e, sl, :]
            pull = None
            for p, (b_j, a_j, q_j) in enumerate(cols):
                g = lax.dot_general(x_t, b_j, (((1,), (1,)), ((), ())), preferred_element_type=jnp.float32)
                w = jnp.exp2(jnp.minimum(g * scale - a_t - a_j, 0.0)) * (q_t * q_j)
                if masked and p == t:
                    diag = lax.broadcasted_iota(jnp.int32, (TILE, TILE), 0) == lax.broadcasted_iota(jnp.int32, (TILE, TILE), 1)
                    w = jnp.where(diag, 0.0, w)
                for h in range(per):
                    rho_t = rho_t + w[:, h * LANES:(h + 1) * LANES]
                part = jnp.dot(w.astype(jnp.bfloat16), b_j, preferred_element_type=jnp.float32)
                pull = part if pull is None else pull + part
            pull = acc[e, sl, :] + pull
            rho[e, sl, :] = rho_t
            if finish is None:
                acc[e, sl, :] = pull
            else:
                finish(sl, force(e, sl, rho_t, pull))

    def force(e, sl, rho_t, pull):
        rho_sum = jnp.sum(rho_t, axis=1, keepdims=True)
        return (rho_sum * xg[e, me, sl, :].astype(jnp.float32) - pull) / feat

    barrier = pltpu.get_barrier_semaphore()
    for i in range(1, n):
        pl.semaphore_signal(barrier, inc=1, device_id={"blk": lax.rem(me + i, n)}, device_id_type=MESH)
    first = [load(which, 0, TILE) for which in range(2)]
    others = [load(which, TILE, rows - TILE) for which in range(2)]
    for copy in first:
        copy.start()
    q_load = pltpu.make_async_copy(q_hbm, q_ref, q_sem)
    rho[...] = jnp.zeros_like(rho)
    for copy in others:
        copy.start()
    q_load.start()
    acc[...] = jnp.zeros_like(acc)
    for k in range(tiles):
        sl = tile_rows(k)
        if k < 2:
            for copy in (first, others)[k]:
                copy.wait()
        x0 = xs[sl, :]
        x1 = x0 + STEP * vs[sl, :]
        xg[1, me, sl, :] = x1.astype(jnp.bfloat16)
        xg[0, me, sl, :] = x0.astype(jnp.bfloat16)
        xs[sl, :] = x1
        if k == 0:
            pl.semaphore_wait(barrier, n - 1)
            for copy in own_copies(1, k):
                copy.start()
    q_load.wait()
    mg[me, 2] = q_ref[...]
    for k in range(tiles * per):
        sl = slice(k * LANES, (k + 1) * LANES)
        for e in (1, 0):
            b = xg[e, me, sl, :].astype(jnp.float32)
            s = jnp.sum(b * b, axis=1, keepdims=True) * (LOG2E / (2.0 * feat))
            wide = jnp.broadcast_to(s, (LANES, LANES))
            aw[e, sl, :] = wide
            mg[me, e, k:k + 1, :] = wide.T[0:1, :]
    for k in range(1, tiles):
        for copy in own_copies(1, k):
            copy.start()
        if k == 1:
            for copy in own_meta():
                copy.start()
    for k in range(tiles):
        for copy in own_copies(0, k):
            copy.start()
    for k in range(tiles * per):
        qw[k * LANES:(k + 1) * LANES, :] = jnp.broadcast_to(q_ref[k:k + 1, :], (LANES, LANES)).T

    @pl.loop(0, 2)
    def _(i):
        pair_tiles(1 - i, [tile(me, k) for k in range(tiles)], masked=True)

    meta_arrived(1, SIB)

    @pl.loop(0, 2)
    def _(i):
        e = 1 - i
        tiles_arrived(tiles, sib_recv.at[e])
        pair_tiles(e, [tile(sib, k) for k in range(tiles)])

    def receive_sides(i):
        e, k = 1 - i // tiles, lax.rem(i, tiles)
        tiles_arrived(2, side_recv.at[e, k])
        fwd_left(e, k).start()
        fwd_right(e, k).start()

        @pl.when(k < half)
        def _():
            for copy in pass_right(e, k):
                copy.start()

        @pl.when(k >= half)
        def _():
            for copy in pass_left(e, k):
                copy.start()

    def relayed_sides(e, k):
        tiles_arrived(2, side_sib_recv.at[e, k])
        return [tile(left_sib, k), tile(right_sib, k)]

    def receive_opposite(e, s):
        tiles_arrived(1, opp_recv.at[e, s])
        for r in opposite_strips(s):
            strip_copy(e, r, opp, sib, opp_sib_recv.at[e, s]).start()

    def relayed_opposite(e, s):
        tiles_arrived(1, opp_sib_recv.at[e, s])
        return [opposite_piece(opp_sib, s)]

    meta_arrived(2, SIDES)
    for copy in fwd_meta():
        copy.start()
    meta_arrived(2, SIDES_SIB)

    @pl.loop(0, 2 * tiles)
    def _(i):
        e, k = 1 - i // tiles, lax.rem(i, tiles)
        receive_sides(i)
        sides = [tile(left, k), tile(right, k)]

        @pl.when(k > 0)
        def _():
            pair_tiles(e, sides + relayed_sides(e, k - 1))

        @pl.when(k == 0)
        def _():
            @pl.when(i > 0)
            def _():
                pair_tiles(1, relayed_sides(1, tiles - 1))

            pair_tiles(e, sides)

    def first_finish(sl, f1):
        f1_ref[sl, :] = f1

    def last_finish(sl, f0):
        v1 = vs[sl, :] + STEP * f0
        x2_ref[sl, :] = xs[sl, :] + STEP * v1
        v2_ref[sl, :] = v1 + STEP * f1_ref[sl, :]

    meta_arrived(1, OPP)
    fwd_opp_meta().start()
    receive_opposite(1, 0)

    @pl.loop(0, 2)
    def _(i):
        e = 1 - i

        @pl.when(i == 1)
        def _():
            pair_tiles(1, relayed_opposite(1, strips - 1), finish=first_finish)
            receive_opposite(0, 0)
            part = jnp.zeros((8, LANES), jnp.float32)
            for r in range(rows // 8):
                part = part + rho[1, r * 8:(r + 1) * 8, :]
            esend[...] = part
            ebuf[me] = part
            for p in range(1, n):
                energy_copy(p).start()

        pair_tiles(e, [opposite_piece(opp, 0)])

        @pl.when(i == 0)
        def _():
            pair_tiles(0, relayed_sides(0, tiles - 1))
            meta_arrived(1, OPP_SIB)

        @pl.loop(1, strips)
        def _(s):
            receive_opposite(e, s)
            pair_tiles(e, [opposite_piece(opp, s)] + relayed_opposite(e, s - 1))

    pair_tiles(0, relayed_opposite(0, strips - 1), finish=last_finish)
    parts = remote(ebuf.at[pl.ds(0, n - 1)], sib, e_sent, e_recv)
    parts.wait_recv()
    e_ref[...] = ebuf[...]
    parts.wait_send()
    remote(xg.at[:, pl.ds(0, n - 1)], sib, sent, sib_recv.at[0]).wait_send()
    remote(mg.at[pl.ds(0, n - 1)], sib, meta_sent, meta_recv.at[0]).wait_send()


def write_out(f1_ref, x2_ref, v2_ref, parts_ref, f1_hbm, e_hbm, x2_hbm, v2_hbm, e_ref, sem):
    copies = [pltpu.make_async_copy(src, dst, sem.at[i])
              for i, (src, dst) in enumerate(((f1_ref, f1_hbm), (x2_ref, x2_hbm), (v2_ref, v2_hbm), (e_ref, e_hbm)))]
    for copy in copies[:3]:
        copy.start()
    total = parts_ref[0]
    for b in range(1, parts_ref.shape[0]):
        total = total + parts_ref[b]
    e_ref[0] = 0.5 * jnp.sum(total)
    copies[3].start()
    for copy in copies:
        copy.wait()


def solution(mesh):
    n = mesh.shape["blk"]
    row_spec = P(("sys", "blk"), None)
    vec_spec = P(("sys", "blk"))

    def local_steps(positions, velocity, charges):
        rows, feat = positions.shape
        tiles = rows // TILE
        block = jax.ShapeDtypeStruct((rows, feat), jnp.float32)
        vmem = pl.BlockSpec(memory_space=pltpu.VMEM)
        hbm = pl.BlockSpec(memory_space=pltpu.HBM)
        dma = pltpu.SemaphoreType.DMA
        parts = pl.pallas_call(
            functools.partial(kernel, n),
            out_shape=(block, block, block, jax.ShapeDtypeStruct((n, 8, LANES), jnp.float32)),
            in_specs=[hbm, hbm, hbm],
            out_specs=(vmem, vmem, vmem, vmem),
            scratch_shapes=[
                pltpu.VMEM((rows, feat), jnp.float32),
                pltpu.VMEM((rows, feat), jnp.float32),
                pltpu.VMEM((rows // LANES, LANES), jnp.float32),
                pltpu.VMEM((2, n, rows, feat), jnp.bfloat16),
                pltpu.VMEM((n, 3, rows // LANES, LANES), jnp.float32),
                pltpu.VMEM((2, rows, LANES), jnp.float32),
                pltpu.VMEM((rows, LANES), jnp.float32),
                pltpu.VMEM((2, rows, feat), jnp.float32),
                pltpu.VMEM((2, rows, LANES), jnp.float32),
                pltpu.VMEM((8, LANES), jnp.float32),
                pltpu.VMEM((n, 8, LANES), jnp.float32),
                dma((2, 2)),
                dma,
                dma,
                dma,
                dma,
                dma((5,)),
                dma,
                dma((2,)),
                dma((2, tiles)),
                dma((2, tiles)),
                dma((2, rows // (2 * LANES))),
                dma((2, rows // (2 * LANES))),
            ],
            compiler_params=pltpu.CompilerParams(collective_id=0, has_side_effects=True, vmem_limit_bytes=52800000),
            cost_estimate=pl.CostEstimate(flops=8 * n * rows * rows * feat, bytes_accessed=20 * rows * feat, transcendentals=2 * n * rows * rows),
        )(*[pltpu.with_memory_space_constraint(x, pltpu.HBM) for x in (positions, velocity, charges.reshape(rows // LANES, LANES))])
        force_one, energy_one, pos_two, vel_two = pl.pallas_call(
            write_out,
            out_shape=(block, jax.ShapeDtypeStruct((1,), jnp.float32), block, block),
            in_specs=[vmem] * 4,
            out_specs=(hbm, hbm, hbm, hbm),
            scratch_shapes=[pltpu.SMEM((1,), jnp.float32), dma((4,))],
            compiler_params=pltpu.CompilerParams(vmem_limit_bytes=2**20),
        )(*parts)
        return force_one, energy_one, pos_two, vel_two

    return jax.shard_map(local_steps, mesh=mesh, in_specs=(row_spec, row_spec, vec_spec), out_specs=(row_spec, P("sys"), row_spec, row_spec), check_vma=False)
```

```python
import functools
import math

import jax
import jax.numpy as jnp
from jax import lax
from jax.experimental import pallas as pl
from jax.experimental.pallas import tpu as pltpu
from jax.sharding import PartitionSpec as P

MESH = pl.DeviceIdType.MESH
STEP = 0.5
LOG2E = math.log2(math.e)
TILE = 256
LANES = 128
SIB, SIDES, SIDES_SIB, OPP, OPP_SIB = range(5)


def kernel(n, x0_hbm, v0_hbm, q_hbm, f1_ref, x2_ref, v2_ref, e_ref,
           xs, vs, q_ref, xg, mg, aw, qw, acc, rho, esend, ebuf,
           load_sem, q_sem, sent, meta_sent, e_sent, meta_recv, e_recv, sib_recv, side_recv, side_sib_recv, opp_recv, opp_sib_recv):
    rows, feat = xs.shape
    tiles = rows // TILE
    per = TILE // LANES
    half = tiles // 2
    strips = half * per
    me = lax.axis_index("blk")
    core = lax.rem(me, 2)
    sib = me + 1 - 2 * core
    right = lax.rem(me + 2, n)
    left = lax.rem(me + n - 2, n)
    opp = lax.rem(me + n // 2, n)
    left_sib = left + 1 - 2 * core
    right_sib = right + 1 - 2 * core
    opp_sib = opp + 1 - 2 * core

    def tile_rows(k):
        return pl.ds(k * TILE, TILE) if isinstance(k, int) else pl.ds(pl.multiple_of(k * TILE, TILE), TILE)

    def remote(ref, dev, send, recv):
        return pltpu.make_async_remote_copy(src_ref=ref, dst_ref=ref, send_sem=send, recv_sem=recv,
                                            device_id={"blk": dev}, device_id_type=MESH)

    def strip_rows(r):
        return pl.ds(r * LANES, LANES) if isinstance(r, int) else pl.ds(pl.multiple_of(r * LANES, LANES), LANES)

    def tile(blk, k):
        return blk, [k * per + p for p in range(per)]

    def opposite_strips(s):
        return s, s + strips

    def opposite_piece(blk, s):
        return blk, opposite_strips(s)

    def strip_copy(e, r, blk, dev, recv):
        return remote(xg.at[e, blk, strip_rows(r), :], dev, sent, recv)

    def block_copy(e, k, blk, dev, recv):
        return remote(xg.at[e, blk, tile_rows(k), :], dev, sent, recv)

    def meta_copy(blk, dev, rel):
        return remote(mg.at[blk], dev, meta_sent, meta_recv.at[rel])

    def own_copies(e, k):
        return (block_copy(e, k, me, right, side_recv.at[e, k]),
                block_copy(e, k, me, left, side_recv.at[e, k]),
                block_copy(e, k, me, sib, sib_recv.at[e]))

    def own_meta():
        return (meta_copy(me, right, SIDES), meta_copy(me, left, SIDES), meta_copy(me, sib, SIB))

    def fwd_left(e, k):
        return block_copy(e, k, left, sib, side_sib_recv.at[e, k])

    def fwd_right(e, k):
        return block_copy(e, k, right, sib, side_sib_recv.at[e, k])

    def pass_right(e, k):
        return [strip_copy(e, k * per + p, left, right, opp_recv.at[e, k * per + p]) for p in range(per)]

    def pass_left(e, k):
        return [strip_copy(e, k * per + p, right, left, opp_recv.at[e, k * per + p - strips]) for p in range(per)]

    def fwd_meta():
        return (meta_copy(left, sib, SIDES_SIB), meta_copy(right, sib, SIDES_SIB),
                remote(mg.at[left, pl.ds(1, 2)], right, meta_sent, meta_recv.at[OPP]),
                remote(mg.at[right, pl.ds(0, 1)], left, meta_sent, meta_recv.at[OPP]))

    def fwd_opp_meta():
        return meta_copy(opp, sib, OPP_SIB)

    def tiles_arrived(count, recv):
        remote(xg.at[0, 0, pl.ds(0, count * TILE), :], sib, sent, recv).wait_recv()

    def meta_arrived(count, rel):
        remote(mg.at[pl.ds(0, count)], sib, meta_sent, meta_recv.at[rel]).wait_recv()

    def energy_copy(i):
        return pltpu.make_async_remote_copy(src_ref=esend, dst_ref=ebuf.at[me], send_sem=e_sent, recv_sem=e_recv,
                                            device_id={"blk": lax.rem(me + i, n)}, device_id_type=MESH)

    def load(which, lo, size):
        src, dst = ((x0_hbm, xs), (v0_hbm, vs))[which]
        part = pl.ds(lo, size)
        return pltpu.make_async_copy(src.at[part, :], dst.at[part, :], load_sem.at[which, 1 if lo else 0])

    def pair_tiles(e, pieces, masked=False, finish=None):
        scale = LOG2E / feat
        cols = []
        for blk, strips in pieces:
            b_j = jnp.concatenate([xg[e, blk, strip_rows(r), :] for r in strips], axis=0)
            a_j = jnp.concatenate([mg[blk, e, pl.ds(r, 1), :] for r in strips], axis=1)
            q_j = jnp.concatenate([mg[blk, 2, pl.ds(r, 1), :] for r in strips], axis=1)
            cols.append((b_j, a_j, q_j))
        for t in range(tiles):
            sl = tile_rows(t)
            x_t = xg[e, me, sl, :]
            a_t = jnp.concatenate([aw[e, sl, :]] * per, axis=1)
            q_t = jnp.concatenate([qw[sl, :]] * per, axis=1)
            rho_t = rho[e, sl, :]
            pull = None
            for p, (b_j, a_j, q_j) in enumerate(cols):
                g = lax.dot_general(x_t, b_j, (((1,), (1,)), ((), ())), preferred_element_type=jnp.float32)
                w = jnp.exp2(jnp.minimum(g * scale - a_t - a_j, 0.0)) * (q_t * q_j)
                if masked and p == t:
                    diag = lax.broadcasted_iota(jnp.int32, (TILE, TILE), 0) == lax.broadcasted_iota(jnp.int32, (TILE, TILE), 1)
                    w = jnp.where(diag, 0.0, w)
                for h in range(per):
                    rho_t = rho_t + w[:, h * LANES:(h + 1) * LANES]
                part = jnp.dot(w.astype(jnp.bfloat16), b_j, preferred_element_type=jnp.float32)
                pull = part if pull is None else pull + part
            pull = acc[e, sl, :] + pull
            rho[e, sl, :] = rho_t
            if finish is None:
                acc[e, sl, :] = pull
            else:
                finish(sl, force(e, sl, rho_t, pull))

    def force(e, sl, rho_t, pull):
        rho_sum = jnp.sum(rho_t, axis=1, keepdims=True)
        return (rho_sum * xg[e, me, sl, :].astype(jnp.float32) - pull) / feat

    barrier = pltpu.get_barrier_semaphore()
    for i in range(1, n):
        pl.semaphore_signal(barrier, inc=1, device_id={"blk": lax.rem(me + i, n)}, device_id_type=MESH)
    first = [load(which, 0, TILE) for which in range(2)]
    others = [load(which, TILE, rows - TILE) for which in range(2)]
    for copy in first:
        copy.start()
    q_load = pltpu.make_async_copy(q_hbm, q_ref, q_sem)
    rho[...] = jnp.zeros_like(rho)
    for copy in others:
        copy.start()
    q_load.start()
    acc[...] = jnp.zeros_like(acc)
    for k in range(tiles):
        sl = tile_rows(k)
        if k < 2:
            for copy in (first, others)[k]:
                copy.wait()
        x0 = xs[sl, :]
        x1 = x0 + STEP * vs[sl, :]
        xg[1, me, sl, :] = x1.astype(jnp.bfloat16)
        xg[0, me, sl, :] = x0.astype(jnp.bfloat16)
        xs[sl, :] = x1
        if k == 0:
            pl.semaphore_wait(barrier, n - 1)
            for copy in own_copies(1, k):
                copy.start()
    q_load.wait()
    mg[me, 2] = q_ref[...]
    for k in range(tiles * per):
        sl = slice(k * LANES, (k + 1) * LANES)
        for e in (1, 0):
            b = xg[e, me, sl, :].astype(jnp.float32)
            s = jnp.sum(b * b, axis=1, keepdims=True) * (LOG2E / (2.0 * feat))
            wide = jnp.broadcast_to(s, (LANES, LANES))
            aw[e, sl, :] = wide
            mg[me, e, k:k + 1, :] = wide.T[0:1, :]
    for k in range(1, tiles):
        for copy in own_copies(1, k):
            copy.start()
        if k == 1:
            for copy in own_meta():
                copy.start()
    for k in range(tiles):
        for copy in own_copies(0, k):
            copy.start()
    for k in range(tiles * per):
        qw[k * LANES:(k + 1) * LANES, :] = jnp.broadcast_to(q_ref[k:k + 1, :], (LANES, LANES)).T

    @pl.loop(0, 2)
    def _(i):
        pair_tiles(1 - i, [tile(me, k) for k in range(tiles)], masked=True)

    meta_arrived(1, SIB)

    @pl.loop(0, 2)
    def _(i):
        e = 1 - i
        tiles_arrived(tiles, sib_recv.at[e])
        pair_tiles(e, [tile(sib, k) for k in range(tiles)])

    def receive_sides(i):
        e, k = 1 - i // tiles, lax.rem(i, tiles)
        tiles_arrived(2, side_recv.at[e, k])
        fwd_left(e, k).start()
        fwd_right(e, k).start()

        @pl.when(k < half)
        def _():
            for copy in pass_right(e, k):
                copy.start()

        @pl.when(k >= half)
        def _():
            for copy in pass_left(e, k):
                copy.start()

    def relayed_sides(e, k):
        tiles_arrived(2, side_sib_recv.at[e, k])
        return [tile(left_sib, k), tile(right_sib, k)]

    def receive_opposite(e, s):
        tiles_arrived(1, opp_recv.at[e, s])
        for r in opposite_strips(s):
            strip_copy(e, r, opp, sib, opp_sib_recv.at[e, s]).start()

    def relayed_opposite(e, s):
        tiles_arrived(1, opp_sib_recv.at[e, s])
        return [opposite_piece(opp_sib, s)]

    meta_arrived(2, SIDES)
    for copy in fwd_meta():
        copy.start()
    meta_arrived(2, SIDES_SIB)

    @pl.loop(0, 2 * tiles)
    def _(i):
        e, k = 1 - i // tiles, lax.rem(i, tiles)
        receive_sides(i)
        sides = [tile(left, k), tile(right, k)]

        @pl.when(k > 0)
        def _():
            pair_tiles(e, sides + relayed_sides(e, k - 1))

        @pl.when(k == 0)
        def _():
            @pl.when(i > 0)
            def _():
                pair_tiles(1, relayed_sides(1, tiles - 1))

            pair_tiles(e, sides)

    def first_finish(sl, f1):
        f1_ref[sl, :] = f1

    def last_finish(sl, f0):
        v1 = vs[sl, :] + STEP * f0
        x2_ref[sl, :] = xs[sl, :] + STEP * v1
        v2_ref[sl, :] = v1 + STEP * f1_ref[sl, :]

    meta_arrived(1, OPP)
    fwd_opp_meta().start()
    receive_opposite(1, 0)

    @pl.loop(0, 2)
    def _(i):
        e = 1 - i

        @pl.when(i == 0)
        def _():
            pair_tiles(1, [opposite_piece(opp, 0)])
            pair_tiles(0, relayed_sides(0, tiles - 1))
            meta_arrived(1, OPP_SIB)

        @pl.when(i == 1)
        def _():
            relayed = relayed_opposite(1, strips - 1)
            receive_opposite(0, 0)
            pair_tiles(1, relayed, finish=first_finish)
            pair_tiles(0, [opposite_piece(opp, 0)])
            sums = [rho[1, r * 8:(r + 1) * 8, :] for r in range(4)]
            for r in range(4, rows // 8):
                sums[r % 4] = sums[r % 4] + rho[1, r * 8:(r + 1) * 8, :]
            part = (sums[0] + sums[1]) + (sums[2] + sums[3])
            esend[...] = part
            ebuf[me] = part
            for p in range(1, n):
                energy_copy(p).start()

        @pl.loop(1, strips)
        def _(s):
            receive_opposite(e, s)
            pair_tiles(e, [opposite_piece(opp, s)] + relayed_opposite(e, s - 1))

    pair_tiles(0, relayed_opposite(0, strips - 1), finish=last_finish)
    parts = remote(ebuf.at[pl.ds(0, n - 1)], sib, e_sent, e_recv)
    parts.wait_recv()
    e_ref[...] = ebuf[...]
    parts.wait_send()
    remote(xg.at[:, pl.ds(0, n - 1)], sib, sent, sib_recv.at[0]).wait_send()
    remote(mg.at[pl.ds(0, n - 1)], sib, meta_sent, meta_recv.at[0]).wait_send()


def write_out(f1_ref, x2_ref, v2_ref, parts_ref, f1_hbm, e_hbm, x2_hbm, v2_hbm, e_ref, sem):
    copies = [pltpu.make_async_copy(src, dst, sem.at[i])
              for i, (src, dst) in enumerate(((f1_ref, f1_hbm), (x2_ref, x2_hbm), (v2_ref, v2_hbm), (e_ref, e_hbm)))]
    for copy in copies[:3]:
        copy.start()
    total = parts_ref[0]
    for b in range(1, parts_ref.shape[0]):
        total = total + parts_ref[b]
    e_ref[0] = 0.5 * jnp.sum(total)
    copies[3].start()
    for copy in copies:
        copy.wait()


def solution(mesh):
    n = mesh.shape["blk"]
    row_spec = P(("sys", "blk"), None)
    vec_spec = P(("sys", "blk"))

    def local_steps(positions, velocity, charges):
        rows, feat = positions.shape
        tiles = rows // TILE
        block = jax.ShapeDtypeStruct((rows, feat), jnp.float32)
        vmem = pl.BlockSpec(memory_space=pltpu.VMEM)
        hbm = pl.BlockSpec(memory_space=pltpu.HBM)
        dma = pltpu.SemaphoreType.DMA
        parts = pl.pallas_call(
            functools.partial(kernel, n),
            out_shape=(block, block, block, jax.ShapeDtypeStruct((n, 8, LANES), jnp.float32)),
            in_specs=[hbm, hbm, hbm],
            out_specs=(vmem, vmem, vmem, vmem),
            scratch_shapes=[
                pltpu.VMEM((rows, feat), jnp.float32),
                pltpu.VMEM((rows, feat), jnp.float32),
                pltpu.VMEM((rows // LANES, LANES), jnp.float32),
                pltpu.VMEM((2, n, rows, feat), jnp.bfloat16),
                pltpu.VMEM((n, 3, rows // LANES, LANES), jnp.float32),
                pltpu.VMEM((2, rows, LANES), jnp.float32),
                pltpu.VMEM((rows, LANES), jnp.float32),
                pltpu.VMEM((2, rows, feat), jnp.float32),
                pltpu.VMEM((2, rows, LANES), jnp.float32),
                pltpu.VMEM((8, LANES), jnp.float32),
                pltpu.VMEM((n, 8, LANES), jnp.float32),
                dma((2, 2)),
                dma,
                dma,
                dma,
                dma,
                dma((5,)),
                dma,
                dma((2,)),
                dma((2, tiles)),
                dma((2, tiles)),
                dma((2, rows // (2 * LANES))),
                dma((2, rows // (2 * LANES))),
            ],
            compiler_params=pltpu.CompilerParams(collective_id=0, has_side_effects=True, vmem_limit_bytes=52800000),
            cost_estimate=pl.CostEstimate(flops=8 * n * rows * rows * feat, bytes_accessed=20 * rows * feat, transcendentals=2 * n * rows * rows),
        )(*[pltpu.with_memory_space_constraint(x, pltpu.HBM) for x in (positions, velocity, charges.reshape(rows // LANES, LANES))])
        force_one, energy_one, pos_two, vel_two = pl.pallas_call(
            write_out,
            out_shape=(block, jax.ShapeDtypeStruct((1,), jnp.float32), block, block),
            in_specs=[vmem] * 4,
            out_specs=(hbm, hbm, hbm, hbm),
            scratch_shapes=[pltpu.SMEM((1,), jnp.float32), dma((4,))],
            compiler_params=pltpu.CompilerParams(vmem_limit_bytes=2**20),
        )(*parts)
        return force_one, energy_one, pos_two, vel_two

    return jax.shard_map(local_steps, mesh=mesh, in_specs=(row_spec, row_spec, vec_spec), out_specs=(row_spec, P("sys"), row_spec, row_spec), check_vma=False)
```

```python
import functools
import math

import jax
import jax.numpy as jnp
from jax import lax
from jax.experimental import pallas as pl
from jax.experimental.pallas import tpu as pltpu
from jax.sharding import PartitionSpec as P

MESH = pl.DeviceIdType.MESH
STEP = 0.5
LOG2E = math.log2(math.e)
TILE = 256
LANES = 128
SIB, SIDES, SIDES_SIB, OPP, OPP_SIB = range(5)


def kernel(n, x0_hbm, v0_hbm, q_hbm, f1_ref, x2_ref, v2_ref, e_ref,
           xs, vs, q_ref, xg, mg, aw, qw, acc, rho, esend, ebuf,
           load_sem, q_sem, sent, meta_sent, e_sent, meta_recv, e_recv, sib_recv, side_recv, side_sib_recv, opp_recv, opp_sib_recv):
    rows, feat = xs.shape
    tiles = rows // TILE
    per = TILE // LANES
    half = tiles // 2
    strips = half * per
    me = lax.axis_index("blk")
    core = lax.rem(me, 2)
    sib = me + 1 - 2 * core
    right = lax.rem(me + 2, n)
    left = lax.rem(me + n - 2, n)
    opp = lax.rem(me + n // 2, n)
    left_sib = left + 1 - 2 * core
    right_sib = right + 1 - 2 * core
    opp_sib = opp + 1 - 2 * core

    def tile_rows(k):
        return pl.ds(k * TILE, TILE) if isinstance(k, int) else pl.ds(pl.multiple_of(k * TILE, TILE), TILE)

    def remote(ref, dev, send, recv):
        return pltpu.make_async_remote_copy(src_ref=ref, dst_ref=ref, send_sem=send, recv_sem=recv,
                                            device_id={"blk": dev}, device_id_type=MESH)

    def strip_rows(r):
        return pl.ds(r * LANES, LANES) if isinstance(r, int) else pl.ds(pl.multiple_of(r * LANES, LANES), LANES)

    def tile(blk, k):
        return blk, [k * per + p for p in range(per)]

    def opposite_strips(s):
        return s, s + strips

    def opposite_piece(blk, s):
        return blk, opposite_strips(s)

    def strip_copy(e, r, blk, dev, recv):
        return remote(xg.at[e, blk, strip_rows(r), :], dev, sent, recv)

    def block_copy(e, k, blk, dev, recv):
        return remote(xg.at[e, blk, tile_rows(k), :], dev, sent, recv)

    def meta_copy(blk, dev, rel):
        return remote(mg.at[blk], dev, meta_sent, meta_recv.at[rel])

    def own_copies(e, k):
        return (block_copy(e, k, me, right, side_recv.at[e, k]),
                block_copy(e, k, me, left, side_recv.at[e, k]),
                block_copy(e, k, me, sib, sib_recv.at[e]))

    def own_meta():
        return (meta_copy(me, right, SIDES), meta_copy(me, left, SIDES), meta_copy(me, sib, SIB))

    def fwd_left(e, k):
        return block_copy(e, k, left, sib, side_sib_recv.at[e, k])

    def fwd_right(e, k):
        return block_copy(e, k, right, sib, side_sib_recv.at[e, k])

    def pass_right(e, k):
        return [strip_copy(e, k * per + p, left, right, opp_recv.at[e, k * per + p]) for p in range(per)]

    def pass_left(e, k):
        return [strip_copy(e, k * per + p, right, left, opp_recv.at[e, k * per + p - strips]) for p in range(per)]

    def fwd_meta():
        return (meta_copy(left, sib, SIDES_SIB), meta_copy(right, sib, SIDES_SIB),
                remote(mg.at[left, pl.ds(1, 2)], right, meta_sent, meta_recv.at[OPP]),
                remote(mg.at[right, pl.ds(0, 1)], left, meta_sent, meta_recv.at[OPP]))

    def fwd_opp_meta():
        return meta_copy(opp, sib, OPP_SIB)

    def tiles_arrived(count, recv):
        remote(xg.at[0, 0, pl.ds(0, count * TILE), :], sib, sent, recv).wait_recv()

    def meta_arrived(count, rel):
        remote(mg.at[pl.ds(0, count)], sib, meta_sent, meta_recv.at[rel]).wait_recv()

    def energy_copy(i):
        return pltpu.make_async_remote_copy(src_ref=esend, dst_ref=ebuf.at[me], send_sem=e_sent, recv_sem=e_recv,
                                            device_id={"blk": lax.rem(me + i, n)}, device_id_type=MESH)

    def load(which, lo, size):
        src, dst = ((x0_hbm, xs), (v0_hbm, vs))[which]
        part = pl.ds(lo, size)
        return pltpu.make_async_copy(src.at[part, :], dst.at[part, :], load_sem.at[which, 1 if lo else 0])

    def pair_tiles(e, pieces, masked=False, finish=None):
        scale = LOG2E / feat
        cols = []
        for blk, strips in pieces:
            b_j = jnp.concatenate([xg[e, blk, strip_rows(r), :] for r in strips], axis=0)
            a_j = jnp.concatenate([mg[blk, e, pl.ds(r, 1), :] for r in strips], axis=1)
            q_j = jnp.concatenate([mg[blk, 2, pl.ds(r, 1), :] for r in strips], axis=1)
            cols.append((b_j, a_j, q_j))
        for t in range(tiles):
            sl = tile_rows(t)
            x_t = xg[e, me, sl, :]
            a_t = jnp.concatenate([aw[e, sl, :]] * per, axis=1)
            q_t = jnp.concatenate([qw[sl, :]] * per, axis=1)
            rho_t = rho[e, sl, :]
            pull = None
            for p, (b_j, a_j, q_j) in enumerate(cols):
                g = lax.dot_general(x_t, b_j, (((1,), (1,)), ((), ())), preferred_element_type=jnp.float32)
                w = jnp.exp2(jnp.minimum(g * scale - a_t - a_j, 0.0)) * (q_t * q_j)
                if masked and p == t:
                    diag = lax.broadcasted_iota(jnp.int32, (TILE, TILE), 0) == lax.broadcasted_iota(jnp.int32, (TILE, TILE), 1)
                    w = jnp.where(diag, 0.0, w)
                for h in range(per):
                    rho_t = rho_t + w[:, h * LANES:(h + 1) * LANES]
                part = jnp.dot(w.astype(jnp.bfloat16), b_j, preferred_element_type=jnp.float32)
                pull = part if pull is None else pull + part
            pull = acc[e, sl, :] + pull
            rho[e, sl, :] = rho_t
            if finish is None:
                acc[e, sl, :] = pull
            else:
                finish(sl, force(e, sl, rho_t, pull))

    def force(e, sl, rho_t, pull):
        rho_sum = jnp.sum(rho_t, axis=1, keepdims=True)
        return (rho_sum * xg[e, me, sl, :].astype(jnp.float32) - pull)

    barrier = pltpu.get_barrier_semaphore()
    for i in range(1, n):
        pl.semaphore_signal(barrier, inc=1, device_id={"blk": lax.rem(me + i, n)}, device_id_type=MESH)
    first = [load(which, 0, TILE) for which in range(2)]
    others = [load(which, TILE, rows - TILE) for which in range(2)]
    for copy in first:
        copy.start()
    q_load = pltpu.make_async_copy(q_hbm, q_ref, q_sem)
    rho[...] = jnp.zeros_like(rho)
    for copy in others:
        copy.start()
    q_load.start()
    acc[...] = jnp.zeros_like(acc)
    for k in range(tiles):
        sl = tile_rows(k)
        if k < 2:
            for copy in (first, others)[k]:
                copy.wait()
        x0 = xs[sl, :]
        x1 = x0 + STEP * vs[sl, :]
        xg[1, me, sl, :] = x1.astype(jnp.bfloat16)
        xg[0, me, sl, :] = x0.astype(jnp.bfloat16)
        xs[sl, :] = x1
        if k == 0:
            pl.semaphore_wait(barrier, n - 1)
            for copy in own_copies(1, k):
                copy.start()
    q_load.wait()
    mg[me, 2] = q_ref[...]
    for k in range(tiles * per):
        sl = slice(k * LANES, (k + 1) * LANES)
        for e in (1, 0):
            b = xg[e, me, sl, :].astype(jnp.float32)
            s = jnp.sum(b * b, axis=1, keepdims=True) * (LOG2E / (2.0 * feat))
            wide = jnp.broadcast_to(s, (LANES, LANES))
            aw[e, sl, :] = wide
            mg[me, e, k:k + 1, :] = wide.T[0:1, :]
    for k in range(1, tiles):
        for copy in own_copies(1, k):
            copy.start()
        if k == 1:
            for copy in own_meta():
                copy.start()
    for k in range(tiles):
        for copy in own_copies(0, k):
            copy.start()
    for k in range(tiles * per):
        qw[k * LANES:(k + 1) * LANES, :] = jnp.broadcast_to(q_ref[k:k + 1, :], (LANES, LANES)).T

    @pl.loop(0, 2)
    def _(i):
        pair_tiles(1 - i, [tile(me, k) for k in range(tiles)], masked=True)

    meta_arrived(1, SIB)

    @pl.loop(0, 2)
    def _(i):
        e = 1 - i
        tiles_arrived(tiles, sib_recv.at[e])
        pair_tiles(e, [tile(sib, k) for k in range(tiles)])

    def receive_sides(i):
        e, k = 1 - i // tiles, lax.rem(i, tiles)
        tiles_arrived(2, side_recv.at[e, k])
        fwd_left(e, k).start()
        fwd_right(e, k).start()

        @pl.when(k < half)
        def _():
            for copy in pass_right(e, k):
                copy.start()

        @pl.when(k >= half)
        def _():
            for copy in pass_left(e, k):
                copy.start()

    def relayed_sides(e, k):
        tiles_arrived(2, side_sib_recv.at[e, k])
        return [tile(left_sib, k), tile(right_sib, k)]

    def receive_opposite(e, s):
        tiles_arrived(1, opp_recv.at[e, s])
        for r in opposite_strips(s):
            strip_copy(e, r, opp, sib, opp_sib_recv.at[e, s]).start()

    def relayed_opposite(e, s):
        tiles_arrived(1, opp_sib_recv.at[e, s])
        return [opposite_piece(opp_sib, s)]

    meta_arrived(2, SIDES)
    for copy in fwd_meta():
        copy.start()
    meta_arrived(2, SIDES_SIB)

    @pl.loop(0, 2 * tiles)
    def _(i):
        e, k = 1 - i // tiles, lax.rem(i, tiles)
        receive_sides(i)
        sides = [tile(left, k), tile(right, k)]

        @pl.when(k > 0)
        def _():
            pair_tiles(e, sides + relayed_sides(e, k - 1))

        @pl.when(k == 0)
        def _():
            @pl.when(i > 0)
            def _():
                pair_tiles(1, relayed_sides(1, tiles - 1))

            pair_tiles(e, sides)

    def first_finish(sl, f1):
        f1_ref[sl, :] = f1 * (1.0 / feat)

    def last_finish(sl, f0):
        v1 = vs[sl, :] + (STEP / feat) * f0
        x2_ref[sl, :] = xs[sl, :] + STEP * v1
        v2_ref[sl, :] = v1 + STEP * f1_ref[sl, :]

    meta_arrived(1, OPP)
    fwd_opp_meta().start()
    receive_opposite(1, 0)

    @pl.loop(0, 2)
    def _(i):
        e = 1 - i

        @pl.when(i == 0)
        def _():
            pair_tiles(1, [opposite_piece(opp, 0)])
            pair_tiles(0, relayed_sides(0, tiles - 1))
            meta_arrived(1, OPP_SIB)

        @pl.when(i == 1)
        def _():
            relayed = relayed_opposite(1, strips - 1)
            receive_opposite(0, 0)
            pair_tiles(1, relayed, finish=first_finish)
            pair_tiles(0, [opposite_piece(opp, 0)])
            sums = [rho[1, r * 8:(r + 1) * 8, :] for r in range(4)]
            for r in range(4, rows // 8):
                sums[r % 4] = sums[r % 4] + rho[1, r * 8:(r + 1) * 8, :]
            part = (sums[0] + sums[1]) + (sums[2] + sums[3])
            esend[...] = part
            ebuf[me] = part
            for p in range(1, n):
                energy_copy(p).start()

        @pl.loop(1, strips)
        def _(s):
            receive_opposite(e, s)
            pair_tiles(e, [opposite_piece(opp, s)] + relayed_opposite(e, s - 1))

    pair_tiles(0, relayed_opposite(0, strips - 1), finish=last_finish)
    parts = remote(ebuf.at[pl.ds(0, n - 1)], sib, e_sent, e_recv)
    parts.wait_recv()
    e_ref[...] = ebuf[...]
    parts.wait_send()
    remote(xg.at[:, pl.ds(0, n - 1)], sib, sent, sib_recv.at[0]).wait_send()
    remote(mg.at[pl.ds(0, n - 1)], sib, meta_sent, meta_recv.at[0]).wait_send()


def write_out(f1_ref, x2_ref, v2_ref, parts_ref, f1_hbm, e_hbm, x2_hbm, v2_hbm, e_ref, sem):
    copies = [pltpu.make_async_copy(src, dst, sem.at[i])
              for i, (src, dst) in enumerate(((f1_ref, f1_hbm), (x2_ref, x2_hbm), (v2_ref, v2_hbm), (e_ref, e_hbm)))]
    for copy in copies[:3]:
        copy.start()
    total = parts_ref[0]
    for b in range(1, parts_ref.shape[0]):
        total = total + parts_ref[b]
    e_ref[0] = 0.5 * jnp.sum(total)
    copies[3].start()
    for copy in copies:
        copy.wait()


def solution(mesh):
    n = mesh.shape["blk"]
    row_spec = P(("sys", "blk"), None)
    vec_spec = P(("sys", "blk"))

    def local_steps(positions, velocity, charges):
        rows, feat = positions.shape
        tiles = rows // TILE
        block = jax.ShapeDtypeStruct((rows, feat), jnp.float32)
        vmem = pl.BlockSpec(memory_space=pltpu.VMEM)
        hbm = pl.BlockSpec(memory_space=pltpu.HBM)
        dma = pltpu.SemaphoreType.DMA
        parts = pl.pallas_call(
            functools.partial(kernel, n),
            out_shape=(block, block, block, jax.ShapeDtypeStruct((n, 8, LANES), jnp.float32)),
            in_specs=[hbm, hbm, hbm],
            out_specs=(vmem, vmem, vmem, vmem),
            scratch_shapes=[
                pltpu.VMEM((rows, feat), jnp.float32),
                pltpu.VMEM((rows, feat), jnp.float32),
                pltpu.VMEM((rows // LANES, LANES), jnp.float32),
                pltpu.VMEM((2, n, rows, feat), jnp.bfloat16),
                pltpu.VMEM((n, 3, rows // LANES, LANES), jnp.float32),
                pltpu.VMEM((2, rows, LANES), jnp.float32),
                pltpu.VMEM((rows, LANES), jnp.float32),
                pltpu.VMEM((2, rows, feat), jnp.float32),
                pltpu.VMEM((2, rows, LANES), jnp.float32),
                pltpu.VMEM((8, LANES), jnp.float32),
                pltpu.VMEM((n, 8, LANES), jnp.float32),
                dma((2, 2)),
                dma,
                dma,
                dma,
                dma,
                dma((5,)),
                dma,
                dma((2,)),
                dma((2, tiles)),
                dma((2, tiles)),
                dma((2, rows // (2 * LANES))),
                dma((2, rows // (2 * LANES))),
            ],
            compiler_params=pltpu.CompilerParams(collective_id=0, has_side_effects=True, vmem_limit_bytes=52800000),
            cost_estimate=pl.CostEstimate(flops=8 * n * rows * rows * feat, bytes_accessed=20 * rows * feat, transcendentals=2 * n * rows * rows),
        )(*[pltpu.with_memory_space_constraint(x, pltpu.HBM) for x in (positions, velocity, charges.reshape(rows // LANES, LANES))])
        force_one, energy_one, pos_two, vel_two = pl.pallas_call(
            write_out,
            out_shape=(block, jax.ShapeDtypeStruct((1,), jnp.float32), block, block),
            in_specs=[vmem] * 4,
            out_specs=(hbm, hbm, hbm, hbm),
            scratch_shapes=[pltpu.SMEM((1,), jnp.float32), dma((4,))],
            compiler_params=pltpu.CompilerParams(vmem_limit_bytes=2**20),
        )(*parts)
        return force_one, energy_one, pos_two, vel_two

    return jax.shard_map(local_steps, mesh=mesh, in_specs=(row_spec, row_spec, vec_spec), out_specs=(row_spec, P("sys"), row_spec, row_spec), check_vma=False)
```
